32 devices in a mesh: leaf: 8 (over z, x), sub: 4 (over y, core).
Axes of the slice: x: 2, y: 2, z: 4, core: 2. Of those that a mesh axis runs over, the one named last changes fastest.
Arguments:
- probe_rhs: float32 [32, 32768], P(None, ('leaf', 'sub')), may hold values from -22.5 to 22.5
- coords: float32 [3, 32768], P(None, ('leaf', 'sub')), may hold values from -52.7 to 52.7
- near_list: int32 [128, 5], P(('leaf', 'sub')), may hold values from -1 to 127, as said below
- far_leaf_list: int32 [128, 8], P(('leaf', 'sub')), may hold values from -1 to 127, as said below
- far_group_list: int32 [8, 14], P('leaf'), may hold values from -1 to 7, as said below
- leaf_basis: float32 [128, 64, 256], P(('leaf', 'sub')), may hold values from -0.375 to 0.375
- leaf_skeleton: float32 [3, 8192], P(None, ('leaf', 'sub')), may hold values from -52.7 to 52.7
- leaf_transfer: float32 [128, 64, 64], P(('leaf', 'sub')), may hold values from -0.375 to 0.375
- device_transfer: float32 [32, 64, 64], P(('leaf', 'sub')), may hold values from -0.375 to 0.375
- group_skeleton: float32 [3, 512], P(None, 'leaf'), may hold values from -1.5 to 4.5
Outputs:
- solution: float32 [32, 32768], P(None, ('leaf', 'sub'))
- residual: float32 [32, 32768], P(None, ('leaf', 'sub'))
The draws below stay inside these ranges and needn't reach their ends.
Inputs may be any that keep to these rules, and one draw needn't show every extreme that they name: `near_list`: row i names distinct leaves within 2 of i, always i itself, -1 in unused slots, in any order; j is named in row i exactly when i is named in row j. `far_leaf_list`: row i names distinct leaves of the same group of 16 consecutive leaves, each more than 2 away from i, -1 in unused slots, in any order; the relation is symmetric. `far_group_list`: row g names distinct groups other than g, -1 in unused slots, in any order; the relation is symmetric.
All inputs are finite; a program needn't handle non-finite values.
Results may differ from the reference program's by a relative error of at most 0.0003.
Values sent between devices are 32-bit elements; how exact they have to be, the bound alone decides.
No kernel may reach another device: no remote copies, remote signals or barrier semaphores. Data moves between devices by JAX's collectives and lax.ppermute only.
A program may use at most 64 MiB of HBM per device.

```python
from functools import partial
import jax
import jax.numpy as jnp
from jax import lax

LEAF = 256
RANK = 64
PROBES = 32
REACH = 2
FAR_LEAF = 8
ITERS = 2
LEAVES_DEV = 4
GROUP_LEAVES = 16
NLEAF = 128
NPTS = 32768
NGROUP = 8
FAR_GROUP = 14
N_SUB = 4
DEVICES = 32


def leaf_centers(key):
    steps_drawn = jax.random.uniform(jax.random.fold_in(key, 11), (3, NLEAF), jnp.float32, -0.4, 0.4)
    return jnp.cumsum(steps_drawn, axis=1)


def jitter_points(key, salt, count):
    return jnp.clip(0.5 * jax.random.normal(jax.random.fold_in(key, salt), (3, NLEAF, count), jnp.float32), -1.5, 1.5)


def draw_coords(key, part):
    centers = leaf_centers(key)
    return (centers[:, :, None] + jitter_points(key, 21, LEAF)).reshape(3, NPTS)


def draw_leaf_skeleton(key, part):
    centers = leaf_centers(key)
    return (centers[:, :, None] + jitter_points(key, 22, RANK)).reshape(3, NLEAF * RANK)


def draw_group_skeleton(key, part):
    centers = jax.random.uniform(jax.random.fold_in(key, 23), (3, NGROUP, 1), jnp.float32, 0.0, 3.0)
    jitter = jnp.clip(0.5 * jax.random.normal(jax.random.fold_in(key, 24), (3, NGROUP, RANK), jnp.float32), -1.5, 1.5)
    return (centers + jitter).reshape(3, NGROUP * RANK)


def draw_probe_rhs(key, part):
    rising = jnp.exp(jnp.log(3.0) * jnp.arange(NLEAF, dtype=jnp.float32) / NLEAF)
    rough = jax.random.uniform(jax.random.fold_in(key, 31), (NLEAF,), jnp.float32, 0.5, 1.5)
    scales = (rising * rough)[None, :, None]
    values = jnp.clip(jax.random.normal(jax.random.fold_in(key, 32), (PROBES, NLEAF, LEAF), jnp.float32), -5.0, 5.0)
    return (scales * values).reshape(PROBES, NPTS)


def pair_table(key, count, block, offsets, salt):
    positions = jnp.arange(count, dtype=jnp.int32)
    in_block = positions % block
    columns = []
    for column_index in range(offsets.shape[0]):
        offset = offsets[column_index]
        kept_pair = jax.random.randint(jax.random.fold_in(key, salt + column_index), (count,), 0, 4) > 0
        upper = jnp.where(kept_pair & (in_block + offset < block), positions + offset, -1)
        earlier = jnp.roll(kept_pair, offset)
        lower = jnp.where(earlier & (in_block - offset >= 0), positions - offset, -1)
        columns = columns + [upper, lower]
    return jnp.stack(columns, axis=1).astype(jnp.int32)


def draw_near_list(key, part):
    offsets = jnp.arange(1, REACH + 1, dtype=jnp.int32)
    table = pair_table(key, NLEAF, NLEAF, offsets, 100)
    itself = jnp.arange(NLEAF, dtype=jnp.int32)[:, None]
    table = jnp.concatenate([itself, table], axis=1)
    return jax.random.permutation(jax.random.fold_in(key, 101), table, axis=1, independent=True)


def draw_far_leaf_list(key, part):
    offsets = (jax.random.permutation(jax.random.fold_in(key, 200), GROUP_LEAVES - REACH - 1)[:FAR_LEAF // 2] + REACH + 1).astype(jnp.int32)
    table = pair_table(key, NLEAF, GROUP_LEAVES, offsets, 300)
    return jax.random.permutation(jax.random.fold_in(key, 301), table, axis=1, independent=True)


def draw_far_group_list(key, part):
    shuffled = (jax.random.permutation(jax.random.fold_in(key, 400), NGROUP - 1) + 1).astype(jnp.int32)
    places = jnp.arange(NGROUP - 1, dtype=jnp.int32)
    priority = jnp.where(shuffled == 1, -2, jnp.where(shuffled == NGROUP // 2, -1, places)).astype(jnp.int32)
    ordering = jnp.argsort(priority, stable=True)
    offsets = shuffled[ordering][:FAR_GROUP // 2].astype(jnp.int32)
    table = pair_table(key, NGROUP, NGROUP, offsets, 500)
    return jax.random.permutation(jax.random.fold_in(key, 501), table, axis=1, independent=True)


def block_scale(key, dims, split, least, high):
    def one(axis_at, parts):
        heights = jax.random.uniform(jax.random.fold_in(jax.random.fold_in(key, 6), axis_at), (parts,), jnp.float32, least / len(split), high / len(split))
        return jnp.repeat(jnp.exp(heights), dims[axis_at] // parts).reshape((-1,) + (1,) * (len(dims) - axis_at - 1))

    level = one(*split[0])
    for cut in split[1:]:
        level = level * one(*cut)
    return level


def centred(own_key, shape, deviation, most, shards=(), kind=jnp.bfloat16):
    entries = deviation * jax.random.normal(own_key, shape, jnp.float32)
    if shards:
        entries = entries * block_scale(own_key, shape, shards, -0.22, 0.18)
    return jnp.clip(entries, -most, most).astype(kind)


def setup_inputs(seed: int = 0) -> dict:
    splits = jax.random.split(jax.random.key(seed), 11)
    probe_rhs = draw_probe_rhs(jax.random.fold_in(splits[10], 71), 0)
    coords = draw_coords(jax.random.fold_in(splits[10], 71), 0)
    near_list = draw_near_list(jax.random.fold_in(splits[10], 71), 0)
    far_leaf_list = draw_far_leaf_list(jax.random.fold_in(splits[10], 71), 0)
    far_group_list = draw_far_group_list(jax.random.fold_in(splits[10], 71), 0)
    leaf_basis = centred(splits[5], (NLEAF, RANK, LEAF), LEAF ** -0.5, 0.375, ((0, 32),), jnp.float32)
    leaf_skeleton = draw_leaf_skeleton(jax.random.fold_in(splits[10], 71), 0)
    leaf_transfer = centred(splits[7], (NLEAF, RANK, RANK), (RANK * LEAVES_DEV) ** -0.5, 0.375, ((0, 32),), jnp.float32)
    device_transfer = centred(splits[8], (DEVICES, RANK, RANK), (RANK * N_SUB) ** -0.5, 0.375, ((0, 32),), jnp.float32)
    group_skeleton = draw_group_skeleton(jax.random.fold_in(splits[10], 71), 0)
    return dict(probe_rhs=probe_rhs, coords=coords, near_list=near_list, far_leaf_list=far_leaf_list, far_group_list=far_group_list, leaf_basis=leaf_basis, leaf_skeleton=leaf_skeleton, leaf_transfer=leaf_transfer, device_transfer=device_transfer, group_skeleton=group_skeleton)


NOISE = 1.0
ROOT_FIVE = 5.0 ** 0.5
HIGHEST = lax.Precision.HIGHEST

def matern(left_points, right_points):
    spread = left_points[..., :, :, None] - right_points[..., :, None, :]
    scaled = ROOT_FIVE * jnp.sqrt(lax.optimization_barrier(jnp.sum(spread * spread, axis=-3)))
    return (1.0 + scaled + scaled * scaled / 3.0) * jnp.exp(-scaled)

def apply_operator(vectors, coords, near_list, far_leaf_list, far_group_list, leaf_basis, leaf_skeleton, leaf_transfer, device_transfer, group_skeleton):
    leaves = near_list.shape[0]
    groups = far_group_list.shape[0]
    devices = device_transfer.shape[0]
    by_leaf = vectors.reshape(PROBES, leaves, LEAF)
    points = coords.reshape(3, leaves, LEAF)

    def near_leaf(leaf_index):
        own_points = points[:, leaf_index]
        totals = jnp.zeros((PROBES, LEAF), jnp.float32)
        for column in range(near_list.shape[1]):
            partner = near_list[leaf_index, column]
            clamped = jnp.maximum(partner, 0)
            kernel_tile = matern(own_points, points[:, clamped])
            product = jnp.dot(by_leaf[:, clamped], kernel_tile.T, precision=HIGHEST)
            totals = totals + jnp.where(partner >= 0, product, 0.0)
        return totals
    near_part = lax.map(near_leaf, jnp.arange(leaves, dtype=jnp.int32))
    coefficients = jnp.einsum('pia,ira->irp', by_leaf, leaf_basis, precision=HIGHEST)
    skeletons = leaf_skeleton.reshape(3, leaves, RANK)

    def far_leaf(leaf_index):
        totals = jnp.zeros((RANK, PROBES), jnp.float32)
        for column in range(far_leaf_list.shape[1]):
            partner = far_leaf_list[leaf_index, column]
            clamped = jnp.maximum(partner, 0)
            kernel_tile = matern(skeletons[:, leaf_index], skeletons[:, clamped])
            product = jnp.dot(kernel_tile, coefficients[clamped], precision=HIGHEST)
            totals = totals + jnp.where(partner >= 0, product, 0.0)
        return totals
    leaf_far = lax.map(far_leaf, jnp.arange(leaves, dtype=jnp.int32))
    device_coef = jnp.einsum('irs,irp->isp', leaf_transfer, coefficients, precision=HIGHEST)
    device_coef = device_coef.reshape(devices, leaves // devices, RANK, PROBES).sum(axis=1)
    group_coef = jnp.einsum('qrs,qrp->qsp', device_transfer, device_coef, precision=HIGHEST)
    group_coef = group_coef.reshape(groups, devices // groups, RANK, PROBES).sum(axis=1)
    group_points = group_skeleton.reshape(3, groups, RANK)

    def far_group(group_index):
        totals = jnp.zeros((RANK, PROBES), jnp.float32)
        for column in range(far_group_list.shape[1]):
            partner = far_group_list[group_index, column]
            clamped = jnp.maximum(partner, 0)
            kernel_tile = matern(group_points[:, group_index], group_points[:, clamped])
            product = jnp.dot(kernel_tile, group_coef[clamped], precision=HIGHEST)
            totals = totals + jnp.where(partner >= 0, product, 0.0)
        return totals
    group_far = lax.map(far_group, jnp.arange(groups, dtype=jnp.int32))
    device_far = jnp.einsum('qrs,qsp->qrp', device_transfer, jnp.repeat(group_far, devices // groups, axis=0), precision=HIGHEST)
    leaf_total = leaf_far + jnp.einsum('irs,isp->irp', leaf_transfer, jnp.repeat(device_far, leaves // devices, axis=0), precision=HIGHEST)
    far_part = jnp.einsum('ira,irp->pia', leaf_basis, leaf_total, precision=HIGHEST)
    near_flat = jnp.transpose(near_part, (1, 0, 2)).reshape(PROBES, -1)
    return NOISE * vectors + near_flat + far_part.reshape(PROBES, -1)

def reference(probe_rhs, coords, near_list, far_leaf_list, far_group_list, leaf_basis, leaf_skeleton, leaf_transfer, device_transfer, group_skeleton):
    operator = partial(apply_operator, coords=coords, near_list=near_list, far_leaf_list=far_leaf_list, far_group_list=far_group_list, leaf_basis=leaf_basis, leaf_skeleton=leaf_skeleton, leaf_transfer=leaf_transfer, device_transfer=device_transfer, group_skeleton=group_skeleton)
    solution = jnp.zeros_like(probe_rhs)
    residual = probe_rhs
    direction = probe_rhs
    norm_now = lax.optimization_barrier(jnp.sum(residual * residual, axis=1))
    for iteration in range(ITERS):
        image_vec = operator(direction)
        step_length = norm_now / lax.optimization_barrier(jnp.sum(direction * image_vec, axis=1))
        solution = solution + step_length[:, None] * direction
        residual = residual - step_length[:, None] * image_vec
        if iteration + 1 < ITERS:
            norm_next = lax.optimization_barrier(jnp.sum(residual * residual, axis=1))
            direction = residual + (norm_next / norm_now)[:, None] * direction
            norm_now = norm_next
    return (solution, residual)
```

```python
import jax
import jax.numpy as jnp
from jax import lax
from jax.experimental import pallas as pl
from jax.experimental.pallas import tpu as pltpu
from jax.sharding import PartitionSpec as P

REACH = 2
NOISE = 1.0
ROOT_FIVE = 5.0**0.5
LOG2_E = 1.4426950408889634
HIGHEST = lax.Precision.HIGHEST
F32 = jnp.float32
BF16 = jnp.bfloat16
DOWN = 2.0**-40
UP = 2.0**20
LANE = 128
EXTRA = 8


def dot(a, b, ca=1, cb=0):
    return lax.dot_general(
        a, b, (((ca,), (cb,)), ((), ())), precision=HIGHEST, preferred_element_type=F32
    )


def dot16(a, b):
    return lax.dot_general(a, b, (((1,), (0,)), ((), ())), preferred_element_type=F32)


def split(x):
    high = x.astype(BF16)
    return high, (x - high.astype(F32)).astype(BF16)


def matern(rows, cols):
    total = None
    for axis in range(3):
        spread = rows[:, axis : axis + 1] - cols[axis : axis + 1, :]
        total = spread * spread if total is None else total + spread * spread
    distance = total * lax.rsqrt(jnp.maximum(total, 1e-35))
    poly = (1.0 + ROOT_FIVE * distance) + (5.0 / 3.0) * total
    return poly * jnp.exp2((-ROOT_FIVE * LOG2_E) * distance)


def named(list_ref, row, index):
    hit = list_ref[row, 0] == index
    for column in range(1, list_ref.shape[1]):
        hit = jnp.logical_or(hit, list_ref[row, column] == index)
    return jnp.where(hit, 1.0, 0.0).astype(F32)


def leaf_coefficients(vec, basis_ref):
    leaves, rank, leaf = basis_ref.shape
    pieces = [
        dot(vec[:, i * leaf : (i + 1) * leaf], basis_ref[i], 1, 1) for i in range(leaves)
    ]
    return jnp.concatenate(pieces, axis=1)


def write_messages(vec, coefs, term, outs, width, rows):
    m1, m2, m3, m4 = outs
    half = REACH * width
    count = vec.shape[1]
    even = lax.axis_index("sub") % 2 == 0
    low = vec[:, :half]
    high = vec[:, count - half :]
    part_a = jnp.where(even, high, low)
    part_b = jnp.where(even, low, high)
    span = coefs.shape[1]
    base = m2.shape[1]
    for ref in (m1, m2, m3):
        ref[rows, 0:span] = coefs
        ref[rows, span:base] = term
    m1[rows, base : base + half] = part_a
    m3[rows, base : base + half] = part_b
    m4[rows, :] = part_b


def padded_lanes(x, lanes):
    return jnp.concatenate(
        [x, jnp.zeros((x.shape[0], lanes - x.shape[1]), x.dtype)], axis=1
    )


def padded_rows(x, rows):
    return jnp.concatenate(
        [x, jnp.zeros((rows - x.shape[0], x.shape[1]), x.dtype)], axis=0
    )


def first_kernel(vec_ref, coords_ref, skel_ref, gskel_ref, basis_ref, transfer_ref, device_ref, *outs):
    leaf = basis_ref.shape[2]
    probes = vec_ref.shape[0]
    vec = vec_ref[...]
    coefs = leaf_coefficients(vec, basis_ref)
    term = dot(dot(coefs, transfer_ref[...]), device_ref[...])
    term = padded_lanes(term, outs[1].shape[1] - coefs.shape[1])
    write_messages(vec, coefs, term, outs, leaf, slice(0, probes))
    coords = padded_rows(coords_ref[...], EXTRA)
    skel = padded_rows(skel_ref[...], EXTRA)
    gskel = padded_rows(padded_lanes(gskel_ref[...], term.shape[1]), EXTRA)
    write_messages(coords, skel, gskel, outs, leaf, slice(probes, probes + EXTRA))


def halos(r1, r3, r4, rows, base):
    sub = lax.axis_index("sub")
    count = lax.axis_size("sub")
    inner = jnp.logical_and(sub > 0, sub < count - 1)
    from_a = r1[rows, base:]
    from_b = jnp.where(inner, r3[rows, base:], r4[rows, :])
    odd = sub % 2 == 1
    return jnp.where(odd, from_a, from_b), jnp.where(odd, from_b, from_a)


def near_product(vec, low, high, stack_ref, th_ref, tl_ref, leaf, leaves, out_ref):
    probes = vec.shape[0]
    half = REACH * leaf
    count = vec.shape[1]
    for start, block in ((0, low), (half, vec), (half + count, high)):
        top, rest = split(block)
        stack_ref[0:probes, start : start + block.shape[1]] = top
        stack_ref[probes:, start : start + block.shape[1]] = rest
    window = (2 * REACH + 1) * leaf
    for i in range(leaves):
        both = dot16(stack_ref[:, i * leaf : i * leaf + window], th_ref[i])
        more = dot16(stack_ref[0:probes, i * leaf : i * leaf + window], tl_ref[i])
        out_ref[:, i * leaf : (i + 1) * leaf] = (
            NOISE * vec[:, i * leaf : (i + 1) * leaf]
            + (both[0:probes] + both[probes:])
            + more
        )


def far_product(blocks, klh_ref, kll_ref):
    everything = jnp.concatenate(blocks, axis=1)
    high, low = split(everything)
    both = dot16(jnp.concatenate([high, low], axis=0), klh_ref[...])
    probes = everything.shape[0]
    return both[0:probes] + both[probes:] + dot16(high, kll_ref[...])


def tiles_kernel(
    near_ref, far_ref, vec_ref, coords_ref, own, r1, r2, r3, r4,
    th_ref, tl_ref, klh_ref, kll_ref, part_ref, lf_ref,
    points_ref, columns_ref, stack_ref,
):
    leaves = near_ref.shape[0]
    probes, count = vec_ref.shape
    leaf = count // leaves
    half = REACH * leaf
    base = own.shape[1]
    span = klh_ref.shape[1]
    rank = span // leaves
    sub = lax.axis_index("sub")
    subs = lax.axis_size("sub")
    group_first = lax.axis_index("leaf") * subs * leaves
    first = group_first + sub * leaves
    extra = slice(probes, probes + EXTRA)
    low, high = halos(r1, r3, r4, extra, base)
    points_ref[:, 0:half] = low
    points_ref[:, half : half + count] = padded_rows(coords_ref[...], EXTRA)
    points_ref[:, half + count :] = high
    columns_ref[...] = points_ref[...].T
    chunk = 64
    parts = leaf // chunk
    for i in range(leaves):
        cols = points_ref[:, half + i * leaf : half + (i + 1) * leaf]
        for k in range(2 * REACH + 1):
            weight = named(near_ref, i, first + i + k - REACH)

            def body(step, _, i=i, k=k, weight=weight, cols=cols):
                row = pl.multiple_of(k * leaf + step * chunk, chunk)
                source = pl.multiple_of((i + k) * leaf + step * chunk, chunk)
                tile = weight * matern(columns_ref[pl.ds(source, chunk), :], cols)
                top, rest = split(tile)
                th_ref[i, pl.ds(row, chunk), :] = top
                tl_ref[i, pl.ds(row, chunk), :] = rest
                return 0

            lax.fori_loop(0, parts, body, 0)
    messages = (own, r1, r2, r3)
    own_skel = own[extra, 0:span]
    lane_leaf = lax.broadcasted_iota(jnp.int32, (1, span), 1) // rank
    for m, message in enumerate(messages):
        skel = message[extra, 0:span].T
        for j in range(leaves):
            index = group_first + (sub ^ m) * leaves + j
            mask = jnp.zeros((1, span), F32)
            for i in range(leaves):
                mask = jnp.where(lane_leaf == i, named(far_ref, i, index), mask)
            tile = mask * matern(skel[j * rank : (j + 1) * rank], own_skel)
            top, rest = split(tile)
            row = m * span + j * rank
            klh_ref[row : row + rank, :] = top
            kll_ref[row : row + rank, :] = rest
    rows = slice(0, probes)
    vec = vec_ref[...]
    low, high = halos(r1, r3, r4, rows, base)
    near_product(vec, low, high, stack_ref, th_ref, tl_ref, leaf, leaves, part_ref)
    lf_ref[...] = far_product([r[rows, 0:span] for r in messages], klh_ref, kll_ref)


def local_kernel(
    vec_ref, own, r1, r2, r3, r4, th_ref, tl_ref, klh_ref, kll_ref,
    part_ref, lf_ref, stack_ref,
):
    leaves = th_ref.shape[0]
    probes, count = vec_ref.shape
    leaf = count // leaves
    base = own.shape[1]
    span = klh_ref.shape[1]
    rows = slice(0, probes)
    vec = vec_ref[...]
    low, high = halos(r1, r3, r4, rows, base)
    near_product(vec, low, high, stack_ref, th_ref, tl_ref, leaf, leaves, part_ref)
    lf_ref[...] = far_product([r[rows, 0:span] for r in (own, r1, r2, r3)], klh_ref, kll_ref)


def finish_image(part_ref, lf_ref, group_ref, kg_ref, basis_ref, transfer_ref, device_ref):
    leaves, rank, leaf = basis_ref.shape
    groups = group_ref.shape[0]
    probes = part_ref.shape[0]

    def one(m, total):
        return total + dot(group_ref[m, 0:probes, 0:rank], kg_ref[m], 1, 1)

    group_far = lax.fori_loop(
        0, groups, one, jnp.zeros((probes, rank), F32), unroll=groups <= 16
    )
    device_far = dot(group_far, device_ref[...], 1, 1)
    total = lf_ref[...] + dot(device_far, transfer_ref[...], 1, 1)
    pieces = [
        part_ref[:, i * leaf : (i + 1) * leaf]
        + dot(total[:, i * rank : (i + 1) * rank], basis_ref[i])
        for i in range(leaves)
    ]
    return jnp.concatenate(pieces, axis=1)


def middle_kernel(
    list_ref, part_ref, lf_ref, group_ref, gskel_ref, basis_ref, transfer_ref, device_ref,
    image_ref, kg_ref, *outs,
):
    leaves, rank, leaf = basis_ref.shape
    groups = group_ref.shape[0]
    probes = part_ref.shape[0]
    mine = lax.axis_index("leaf")
    own = padded_rows(padded_lanes(gskel_ref[...], LANE), EXTRA).T[0:rank]

    def one(m, _):
        weight = named(list_ref, 0, mine ^ m)
        other = group_ref[m, probes : probes + EXTRA, 0:rank]
        kg_ref[m] = weight * matern(own, other)
        return 0

    lax.fori_loop(0, groups, one, 0, unroll=groups <= 16)
    image = finish_image(part_ref, lf_ref, group_ref, kg_ref, basis_ref, transfer_ref, device_ref)
    image_ref[...] = image
    coefs = leaf_coefficients(image, basis_ref)
    term = dot(dot(coefs, transfer_ref[...]), device_ref[...])
    term = padded_lanes(term, outs[1].shape[1] - coefs.shape[1])
    write_messages(image, coefs, term, outs, leaf, slice(0, probes))


def last_kernel(
    vec_ref, first_ref, part_ref, lf_ref, group_ref, kg_ref, basis_ref, transfer_ref, device_ref,
    second_ref, sums_ref,
):
    probes, count = vec_ref.shape
    second = finish_image(part_ref, lf_ref, group_ref, kg_ref, basis_ref, transfer_ref, device_ref)
    second_ref[...] = second
    vec = vec_ref[...]
    first = first_ref[...]
    ones = jnp.ones((8, count), F32)
    row = lax.broadcasted_iota(jnp.int32, (8, probes), 0)
    products = (vec * vec, vec * first, first * first, (DOWN * first) * second)
    sums = jnp.zeros((8, probes), F32)
    for k, product in enumerate(products):
        sums = jnp.where(row == k, dot(ones, product, 1, 1), sums)
    for k in range(sums_ref.shape[0] // 8):
        sums_ref[8 * k : 8 * k + 8, :] = sums


def update_kernel(sums_ref, vec_ref, first_ref, second_ref, solution_ref, residual_ref):
    gathered = sums_ref[...]
    rows = gathered.shape[0]
    pick = (
        lax.broadcasted_iota(jnp.int32, (rows, LANE), 0) % 8
        == lax.broadcasted_iota(jnp.int32, (rows, LANE), 1)
    ).astype(F32)
    scalars = dot(gathered, pick, 0, 0)
    bb = scalars[:, 0:1]
    bw = scalars[:, 1:2]
    ww = scalars[:, 2:3]
    wv = scalars[:, 3:4]
    step = bb / bw
    rise = (step * ww) * step
    norm = rise - bb
    grow = rise / bb
    scaled = step * UP
    curvature = (grow * grow) * bw - (2.0 * grow) * (step * ww) + (scaled * wv) * scaled
    again = norm / curvature
    vec = vec_ref[...]
    first = first_ref[...]
    second = second_ref[...]
    direction = grow * vec - step * first
    solution_ref[...] = step * vec + again * direction
    residual_ref[...] = (vec - step * first) - again * (grow * first - step * second)


def vmem(count):
    return [pl.BlockSpec(memory_space=pltpu.VMEM)] * count


def smem(count):
    return [pl.BlockSpec(memory_space=pltpu.SMEM)] * count


def shape(*dims, dtype=F32):
    return jax.ShapeDtypeStruct(dims, dtype)


def call(kernel, outs, args, scalars=0, scratch=(), name=None, flops=0):
    return pl.pallas_call(
        kernel,
        out_shape=tuple(outs),
        in_specs=smem(scalars) + vmem(len(args) - scalars),
        out_specs=tuple(vmem(len(outs))),
        scratch_shapes=list(scratch),
        name=name,
        cost_estimate=pl.CostEstimate(flops=flops, transcendentals=0, bytes_accessed=1000000),
    )(*args)


def message_shapes(rows, base, half):
    return [
        shape(rows, base + half),
        shape(rows, base),
        shape(rows, base + half),
        shape(rows, half),
    ]


def exchange(m1, m2, m3, m4):
    subs = lax.axis_size("sub")
    nodes = subs * lax.axis_size("leaf")

    def swap(x, m):
        return lax.ppermute(x, "sub", [(i, i ^ m) for i in range(subs)])

    across = [(q, q + 1) for q in range(subs - 1, nodes - 1, subs)]
    across = across + [(target, source) for source, target in across]
    return swap(m1, 1), swap(m2, 2), swap(m3, 3), lax.ppermute(m4, ("leaf", "sub"), across)


def group_gather(own, r1, r2, r3, span, base):
    groups = lax.axis_size("leaf")
    held = sum(x[:, span:base] for x in (r1, r2, r3)) + own[:, span:base]
    return spread_groups(held[None], groups)


def spread_groups(held, groups):
    bit = 1
    while bit < groups:
        came = lax.ppermute(held, "leaf", [(i, i ^ bit) for i in range(groups)])
        held = jnp.concatenate([held, came], axis=0)
        bit = 2 * bit
    return held


def shards(
    probe_rhs,
    coords,
    near_list,
    far_leaf_list,
    far_group_list,
    leaf_basis,
    leaf_skeleton,
    leaf_transfer,
    device_transfer,
    group_skeleton,
):
    leaves, rank, leaf = leaf_basis.shape
    probes, count = probe_rhs.shape
    groups = lax.axis_size("leaf")
    nodes = groups * lax.axis_size("sub")
    half = REACH * leaf
    span = leaves * rank
    base = span + LANE
    window = (2 * REACH + 1) * leaf
    transfer = leaf_transfer.reshape(span, rank)
    device = device_transfer[0]
    sent = call(
        first_kernel,
        message_shapes(probes + EXTRA, base, half),
        (probe_rhs, coords, leaf_skeleton, group_skeleton, leaf_basis, transfer, device),
        name="coefficients",
    )
    came = exchange(*sent)
    own = sent[1]
    term = own[:probes, span:base] + sum(x[:probes, span:base] for x in came[:3])
    held = jnp.concatenate([term, own[probes:, span:base]], axis=0)
    gathered = spread_groups(held[None], groups)
    th, tl, klh, kll, part, lf = call(
        tiles_kernel,
        [
            shape(leaves, window, leaf, dtype=BF16),
            shape(leaves, window, leaf, dtype=BF16),
            shape(lax.axis_size("sub") * span, span, dtype=BF16),
            shape(lax.axis_size("sub") * span, span, dtype=BF16),
            shape(probes, count),
            shape(probes, span),
        ],
        (near_list, far_leaf_list, probe_rhs, coords, own, *came),
        scalars=2,
        scratch=[
            pltpu.VMEM((EXTRA, count + 2 * half), F32),
            pltpu.VMEM((count + 2 * half, EXTRA), F32),
            pltpu.VMEM((2 * probes, count + 2 * half), BF16),
        ],
        name="tiles",
    )
    image, kg, *sent = call(
        middle_kernel,
        [shape(probes, count), shape(groups, rank, rank)]
        + message_shapes(probes, base, half),
        (far_group_list, part, lf, gathered, group_skeleton, leaf_basis, transfer, device),
        scalars=1,
        name="middle",
    )
    came = exchange(*sent)
    own = sent[1]
    gathered = group_gather(own, came[0], came[1], came[2], span, base)
    part, lf = call(
        local_kernel,
        [shape(probes, count), shape(probes, span)],
        (image, own, *came, th, tl, klh, kll),
        scratch=[pltpu.VMEM((2 * probes, count + 2 * half), BF16)],
        name="local",
    )
    second, sums = call(
        last_kernel,
        [shape(probes, count), shape(8 * nodes, probes)],
        (probe_rhs, image, part, lf, gathered, kg, leaf_basis, transfer, device),
        name="last",
    )
    sums = lax.all_to_all(sums, ("leaf", "sub"), 0, 0, tiled=True)
    return call(
        update_kernel,
        [shape(probes, count), shape(probes, count)],
        (sums, probe_rhs, image, second),
        name="update",
    )


def solution(mesh):
    return jax.shard_map(
        shards,
        mesh=mesh,
        in_specs=(
            P(None, ("leaf", "sub")),
            P(None, ("leaf", "sub")),
            P(("leaf", "sub"), None),
            P(("leaf", "sub"), None),
            P("leaf", None),
            P(("leaf", "sub"), None, None),
            P(None, ("leaf", "sub")),
            P(("leaf", "sub"), None, None),
            P(("leaf", "sub"), None, None),
            P(None, "leaf"),
        ),
        out_specs=(P(None, ("leaf", "sub")), P(None, ("leaf", "sub"))),
        check_vma=False,
    )
```

```python
from functools import partial
import jax
import jax.numpy as jnp
from jax import lax
from jax.experimental import pallas as pl
from jax.experimental.pallas import tpu as pltpu
from jax.sharding import PartitionSpec as P

REACH = 2
NOISE = 1.0
ROOT_FIVE = 5.0**0.5
LOG2_E = 1.4426950408889634
HIGHEST = lax.Precision.HIGHEST
F32 = jnp.float32
BF16 = jnp.bfloat16
DOWN = 2.0**-40
UP = 2.0**20
LANE = 128
EXTRA = 8
CHUNK = 32
GRANT = 16 * 2**20
DENSE = 1024


def dot(a, b, ca=1, cb=0):
    return lax.dot_general(
        a, b, (((ca,), (cb,)), ((), ())), precision=HIGHEST, preferred_element_type=F32
    )


def split(x):
    high = x.astype(BF16)
    return high, (x - high.astype(F32)).astype(BF16)


def stacked(x):
    return jnp.concatenate(split(x), axis=0)


def product(stack, high, low, transposed=False):
    rows = stack.shape[0] // 2
    dims = (((1,), (1 if transposed else 0,)), ((), ()))
    both = lax.dot_general(stack, high, dims, preferred_element_type=F32)
    more = lax.dot_general(stack[:rows], low, dims, preferred_element_type=F32)
    return (both[:rows] + both[rows:]) + more


def matern(rows, cols, weight):
    total = None
    for row, col in zip(rows, cols):
        spread = row - col
        total = spread * spread if total is None else total + spread * spread
    distance = total * lax.rsqrt(jnp.maximum(total, 1e-35))
    poly = (weight + (ROOT_FIVE * weight) * distance) + ((5.0 / 3.0) * weight) * total
    return poly * jnp.exp2((-ROOT_FIVE * LOG2_E) * distance)


def named(list_ref, row, index):
    hit = list_ref[row, 0] == index
    for column in range(1, list_ref.shape[1]):
        hit = jnp.logical_or(hit, list_ref[row, column] == index)
    return jnp.where(hit, 1.0, 0.0).astype(F32)


def padded_lanes(x, lanes):
    return jnp.concatenate(
        [x, jnp.zeros((x.shape[0], lanes - x.shape[1]), x.dtype)], axis=1
    )


def padded_rows(x, rows):
    return jnp.concatenate(
        [x, jnp.zeros((rows - x.shape[0], x.shape[1]), x.dtype)], axis=0
    )


def write_messages(vec, coefs, term, outs, half, rows):
    m1, own, m4 = outs
    count = vec.shape[1]
    even = lax.axis_index("sub") % 2 == 0
    low = vec[:, :half]
    high = vec[:, count - half :]
    span = coefs.shape[1]
    base = own.shape[1]
    for ref in (m1, own):
        ref[rows, 0:span] = coefs
        ref[rows, span:base] = term
    m1[rows, base : base + half] = jnp.where(even, high, low)
    m4[rows, :] = jnp.where(even, low, high)


def halos(r1, r4, rows, base):
    odd = lax.axis_index("sub") % 2 == 1
    from_a = r1[rows, base:]
    from_b = r4[rows, :]
    return jnp.where(odd, from_a, from_b), jnp.where(odd, from_b, from_a)


def first_kernel(
    list_ref, vec_ref, coords_ref, skel_ref, gskel_ref, basis_ref, transfer_ref, device_ref,
    *outs,
):
    leaves, rank, leaf = basis_ref.shape
    probes = vec_ref.shape[0]
    half = REACH * leaf
    vec = vec_ref[...]
    coefs = jnp.concatenate(
        [dot(vec[:, i * leaf : (i + 1) * leaf], basis_ref[i], 1, 1) for i in range(leaves)],
        axis=1,
    )
    term = padded_lanes(dot(dot(coefs, transfer_ref[...]), device_ref[...]), LANE)
    write_messages(vec, coefs, term, outs, half, slice(0, probes))
    relative = lax.axis_index("leaf") ^ lax.broadcasted_iota(jnp.int32, (1, LANE), 1)
    listed = jnp.zeros((1, LANE), F32)
    for column in range(list_ref.shape[1]):
        listed = jnp.where(relative == list_ref[0, column], 1.0, listed)
    group_rows = jnp.concatenate([padded_lanes(gskel_ref[...], LANE), listed], axis=0)
    write_messages(
        padded_rows(coords_ref[...], EXTRA),
        padded_rows(skel_ref[...], EXTRA),
        padded_rows(group_rows, EXTRA),
        outs,
        half,
        slice(probes, probes + EXTRA),
    )


def spread_columns(points, wide_ref):
    columns = points.T
    for axis in range(3):
        wide_ref[axis] = jnp.broadcast_to(
            columns[:, axis : axis + 1], (columns.shape[0], LANE)
        )


def fill_tile(wide_ref, source, points_ref, top_row, lane, width, weight, pair, row, size):
    high_ref, low_ref = pair

    def body(step, _):
        start = pl.multiple_of(source + step * CHUNK, CHUNK)
        target = pl.multiple_of(row + step * CHUNK, CHUNK)
        rows = [wide_ref[axis, pl.ds(start, CHUNK), :] for axis in range(3)]
        for at in range(0, width, LANE):
            cols = [
                points_ref[top_row + axis : top_row + axis + 1, lane + at : lane + at + LANE]
                for axis in range(3)
            ]
            factor = weight[:, at : at + LANE] if weight.ndim else weight
            top, rest = split(matern(rows, cols, factor))
            high_ref[pl.ds(target, CHUNK), at : at + LANE] = top
            low_ref[pl.ds(target, CHUNK), at : at + LANE] = rest
        return 0

    lax.fori_loop(0, size // CHUNK, body, 0, unroll=2)


def window_tiles(leaves):
    inside = []
    across = []
    for i in range(leaves):
        for j in range(i - REACH, i + REACH + 1):
            (inside if 0 <= j < leaves else across).append((i, j))
    return inside, across


def prepare_kernel(
    near_ref, vec_ref, coords_ref, basis_ref, transfer_ref, device_ref,
    th_ref, tl_ref, ubh_ref, ubl_ref, copy_ref, points_ref, wide_ref,
):
    leaves, rank, leaf = basis_ref.shape
    copy_ref[...] = vec_ref[...]
    first = (lax.axis_index("leaf") * lax.axis_size("sub") + lax.axis_index("sub")) * leaves
    points_ref[...] = padded_rows(coords_ref[...], EXTRA)
    spread_columns(points_ref[...], wide_ref)
    for at, (i, j) in enumerate(window_tiles(leaves)[0]):
        fill_tile(
            wide_ref, j * leaf, points_ref, 0, i * leaf, leaf, named(near_ref, i, first + j),
            (th_ref, tl_ref), at * leaf, leaf,
        )
    chain = dot(transfer_ref[...], device_ref[...])
    for i in range(leaves):
        basis = basis_ref[i]
        group_basis = dot(chain[i * rank : (i + 1) * rank], basis, 0, 0)
        top, rest = split(jnp.concatenate([basis, group_basis], axis=0))
        ubh_ref[i] = top
        ubl_ref[i] = rest


def term_kernel(own, r1, r2, r3, out_ref):
    rows = out_ref.shape[0] - EXTRA
    span = own.shape[1] - LANE
    out_ref[rows:, :] = own[rows:, span:]
    out_ref[0:rows, :] = (own[0:rows, span:] + r1[0:rows, span : span + LANE]) + (
        r2[0:rows, span:] + r3[0:rows, span:]
    )


def local_part(vec, low, high, blocks, tiles, bases, out_ref):
    th_ref, tl_ref, hh_ref, hl_ref, klh_ref, kll_ref = tiles
    ubh_ref, ubl_ref = bases
    leaves, double, leaf = ubh_ref.shape
    rank = double // 2
    inside, across = window_tiles(leaves)
    low, own, high = stacked(low), stacked(vec), stacked(high)

    def piece(j):
        if j < 0:
            return low[:, (j + REACH) * leaf : (j + REACH + 1) * leaf]
        if j >= leaves:
            return high[:, (j - leaves) * leaf : (j - leaves + 1) * leaf]
        return own[:, j * leaf : (j + 1) * leaf]

    far = product(stacked(jnp.concatenate(blocks, axis=1)), klh_ref[...], kll_ref[...])
    far_stack = stacked(far)
    near = []
    for i in range(leaves):
        total = NOISE * vec[:, i * leaf : (i + 1) * leaf]
        for pairs, high_ref, low_ref in ((inside, th_ref, tl_ref), (across, hh_ref, hl_ref)):
            at = [n for n, pair in enumerate(pairs) if pair[0] == i]
            if at:
                where = slice(at[0] * leaf, (at[-1] + 1) * leaf)
                wide = jnp.concatenate([piece(pairs[n][1]) for n in at], axis=1)
                total = total + product(wide, high_ref[where, :], low_ref[where, :])
        near.append(total)
        out_ref[:, i * leaf : (i + 1) * leaf] = total + product(
            far_stack[:, i * rank : (i + 1) * rank], ubh_ref[i, 0:rank, :], ubl_ref[i, 0:rank, :]
        )
    return jnp.concatenate(near, axis=1), far


def border_kernel(
    near_ref, far_ref, vec_ref, own, r1, r2, r3, r4, points_ref, th_ref, tl_ref, ubh_ref, ubl_ref,
    hh_ref, hl_ref, klh_ref, kll_ref, part_ref,
    ends_ref, wide_ref, skel_wide_ref,
):
    leaves = near_ref.shape[0]
    probes, count = vec_ref.shape
    leaf = count // leaves
    half = REACH * leaf
    base = own.shape[1]
    span = klh_ref.shape[1]
    rank = span // leaves
    sub = lax.axis_index("sub")
    group_first = lax.axis_index("leaf") * lax.axis_size("sub") * leaves
    first = group_first + sub * leaves
    extra = slice(probes, probes + EXTRA)
    rows = slice(0, probes)
    low, high = halos(r1, r4, extra, base)
    ends_ref[:, 0:half] = low
    ends_ref[:, half:] = high
    spread_columns(ends_ref[...], wide_ref)
    for at, (i, j) in enumerate(window_tiles(leaves)[1]):
        source = (j + REACH) * leaf if j < 0 else half + (j - leaves) * leaf
        fill_tile(
            wide_ref, source, points_ref, 0, i * leaf, leaf, named(near_ref, i, first + j),
            (hh_ref, hl_ref), at * leaf, leaf,
        )
    messages = (own, r1, r2, r3)
    lane_leaf = lax.broadcasted_iota(jnp.int32, (1, span), 1) // rank
    for m, message in enumerate(messages):
        spread_columns(message[extra, 0:span], skel_wide_ref.at[m])
    for m in range(len(messages)):
        for j in range(leaves):
            index = group_first + (sub ^ m) * leaves + j
            mask = jnp.zeros((1, span), F32)
            for i in range(leaves):
                mask = jnp.where(lane_leaf == i, named(far_ref, i, index), mask)
            fill_tile(
                skel_wide_ref.at[m], j * rank, own, probes, 0, span, mask,
                (klh_ref, kll_ref), m * span + j * rank, rank,
            )
    low, high = halos(r1, r4, rows, base)
    local_part(
        vec_ref[...], low, high, [r[rows, 0:span] for r in messages],
        (th_ref, tl_ref, hh_ref, hl_ref, klh_ref, kll_ref), (ubh_ref, ubl_ref), part_ref,
    )


def row_sum(x):
    return jnp.sum(x, axis=1, keepdims=True)


def local_kernel(
    rhs_ref, vec_ref, own, r1, r2, r3, r4, th_ref, tl_ref, hh_ref, hl_ref, klh_ref, kll_ref,
    ubh_ref, ubl_ref, part_ref, message_ref,
):
    base = own.shape[1]
    span = klh_ref.shape[1]
    rank = ubh_ref.shape[1] // 2
    rows = slice(0, vec_ref.shape[0])
    rhs = rhs_ref[...]
    vec = vec_ref[...]
    low, high = halos(r1, r4, rows, base)
    blocks = [r[rows, 0:span] for r in (own, r1, r2, r3)]
    near, far = local_part(
        vec, low, high, blocks,
        (th_ref, tl_ref, hh_ref, hl_ref, klh_ref, kll_ref), (ubh_ref, ubl_ref), part_ref,
    )
    shares = (
        row_sum(rhs * rhs),
        row_sum(rhs * vec),
        row_sum(vec * vec),
        row_sum((DOWN * vec) * near) + row_sum((DOWN * blocks[0]) * far),
    )
    term = (own[:, span:base] + r1[:, span:base]) + (r2[:, span:base] + r3[:, span:base])
    lane = lax.broadcasted_iota(jnp.int32, term.shape, 1)
    for at, share in enumerate(shares):
        term = jnp.where(lane == rank + at, share, term)
    message_ref[...] = term


def group_row(group_ref, rows, rank):
    groups = group_ref.shape[0]
    return jnp.concatenate([group_ref[m, rows, 0:rank] for m in range(groups)], axis=1)


def group_mask(group_ref, row, block, rank):
    groups = group_ref.shape[0]
    listed = group_ref[block, row : row + 1, :]
    lane_group = lax.broadcasted_iota(jnp.int32, (1, groups * rank), 1) // rank
    mask = jnp.zeros((1, groups * rank), F32)
    for m in range(groups):
        mask = jnp.where(lane_group == m, listed[:, block ^ m : (block ^ m) + 1], mask)
    return mask


def middle_kernel(
    part_ref, group_ref, ubh_ref, ubl_ref, image_ref, kgh_ref, kgl_ref, *rest,
):
    outs = rest[:3]
    points_ref, wide_ref = rest[3:]
    leaves, double, leaf = ubh_ref.shape
    rank = double // 2
    groups = group_ref.shape[0]
    probes = part_ref.shape[0]
    points_ref[...] = group_row(group_ref, slice(probes, probes + EXTRA), rank)
    spread_columns(group_ref[0, probes : probes + EXTRA, :], wide_ref)
    fill_tile(
        wide_ref, 0, points_ref, 0, 0, groups * rank,
        group_mask(group_ref, probes + 3, 0, rank), (kgh_ref, kgl_ref), 0, rank,
    )
    held = group_row(group_ref, slice(0, probes), rank)
    group_far = product(stacked(held), kgh_ref[...], kgl_ref[...], True)
    group_stack = stacked(group_far)
    image = []
    coefs = []
    term = None
    for i in range(leaves):
        piece = part_ref[:, i * leaf : (i + 1) * leaf] + product(
            group_stack, ubh_ref[i, rank:, :], ubl_ref[i, rank:, :]
        )
        image.append(piece)
        both = product(stacked(piece), ubh_ref[i], ubl_ref[i], True)
        coefs.append(both[:, :rank])
        term = both if term is None else term + both
    image = jnp.concatenate(image, axis=1)
    image_ref[...] = image
    write_messages(
        image, jnp.concatenate(coefs, axis=1), padded_lanes(term[:, rank:], LANE), outs,
        REACH * leaf, slice(0, probes),
    )


def groups_kernel(group_ref, kah_ref, kal_ref, points_ref, wide_ref):
    groups, rows, _ = group_ref.shape
    rank = kah_ref.shape[0] // groups
    probes = rows - EXTRA
    points_ref[...] = group_row(group_ref, slice(probes, rows), rank)
    spread_columns(points_ref[...], wide_ref)
    for m in range(groups):
        fill_tile(
            wide_ref, m * rank, points_ref, 0, 0, groups * rank,
            group_mask(group_ref, probes + 3, m, rank), (kah_ref, kal_ref), m * rank, rank,
        )


def last_kernel(part_ref, group_ref, kah_ref, kal_ref, ubh_ref, ubl_ref, second_ref, pair_ref):
    leaves, double, leaf = ubh_ref.shape
    rank = double // 2
    probes = part_ref.shape[0]
    held = group_row(group_ref, slice(0, probes), rank)
    far = product(stacked(held), kah_ref[...], kal_ref[...], True)
    group_stack = stacked(far[:, :rank])
    for i in range(leaves):
        second_ref[:, i * leaf : (i + 1) * leaf] = part_ref[:, i * leaf : (i + 1) * leaf] + product(
            group_stack, ubh_ref[i, rank:, :], ubl_ref[i, rank:, :]
        )
    share = row_sum((DOWN * held[:, : far.shape[1]]) * far)
    pair_ref[...] = jnp.broadcast_to(share, (probes, LANE))


def update_kernel(
    rank, own, s1, s2, s3, pair_ref, vec_ref, first_ref, second_ref, solution_ref, residual_ref,
):
    sums = (own[...] + s1[...]) + (s2[...] + s3[...])
    bb, bw, ww, wv = (sums[:, rank + k : rank + k + 1] for k in range(4))
    wv = wv + pair_ref[:, 0:1]
    step = bb / bw
    rise = (step * ww) * step
    norm = rise - bb
    grow = rise / bb
    scaled = step * UP
    curvature = (grow * grow) * bw - (2.0 * grow) * (step * ww) + (scaled * wv) * scaled
    again = norm / curvature
    vec = vec_ref[...]
    first = first_ref[...]
    second = second_ref[...]
    direction = grow * vec - step * first
    solution_ref[...] = step * vec + again * direction
    residual_ref[...] = (vec - step * first) - again * (grow * first - step * second)


def vmem(count):
    return [pl.BlockSpec(memory_space=pltpu.VMEM)] * count


def smem(count):
    return [pl.BlockSpec(memory_space=pltpu.SMEM)] * count


def shape(*dims, dtype=F32):
    return jax.ShapeDtypeStruct(dims, dtype)


def pair(*dims):
    return [shape(*dims, dtype=BF16)] * 2


def call(kernel, outs, args, scalars=0, scratch=(), name=None, flops=0):
    return pl.pallas_call(
        kernel,
        out_shape=tuple(outs),
        in_specs=smem(scalars) + vmem(len(args) - scalars),
        out_specs=tuple(vmem(len(outs))),
        scratch_shapes=[pltpu.VMEM(dims, F32) for dims in scratch],
        name=name,
        compiler_params=pltpu.CompilerParams(vmem_limit_bytes=GRANT),
        cost_estimate=pl.CostEstimate(
            flops=flops, transcendentals=0, bytes_accessed=1000000
        ),
    )(*args)


def swap(x, axis, m):
    return lax.ppermute(x, axis, [(i, i ^ m) for i in range(lax.axis_size(axis))])


def exchange(m1, own, m4):
    nodes = lax.axis_size("sub") * lax.axis_size("leaf")
    across = [(q, q + 1) for q in range(1, nodes - 1, 2)]
    across = across + [(target, source) for source, target in across]
    return (
        swap(m1, "sub", 1),
        swap(own, "sub", 2),
        swap(own, "sub", 3),
        lax.ppermute(m4, ("leaf", "sub"), across),
    )


def spread_groups(held):
    held = held[None]
    bit = 1
    while bit < lax.axis_size("leaf"):
        held = jnp.concatenate([held, swap(held, "leaf", bit)], axis=0)
        bit = 2 * bit
    return held


def far_memory(*args):
    return [pltpu.with_memory_space_constraint(x, pltpu.HBM) for x in args]


def shards(
    probe_rhs,
    coords,
    near_list,
    far_leaf_list,
    far_group_list,
    leaf_basis,
    leaf_skeleton,
    leaf_transfer,
    device_transfer,
    group_skeleton,
):
    leaves, rank, leaf = leaf_basis.shape
    probes, count = probe_rhs.shape
    groups = lax.axis_size("leaf")
    half = REACH * leaf
    span = leaves * rank
    base = span + LANE
    inside, across = window_tiles(leaves)
    transfer = leaf_transfer.reshape(span, rank)
    device = device_transfer[0]

    def messages(rows):
        return [shape(rows, base + half), shape(rows, base), shape(rows, half)]

    sent = call(
        first_kernel,
        messages(probes + EXTRA),
        far_memory(
            far_group_list, probe_rhs, coords, leaf_skeleton, group_skeleton, leaf_basis,
            transfer, device,
        ),
        scalars=1,
        name="coefficients",
    )
    own = sent[1]
    r1, r2, r3, r4 = exchange(*sent)
    th, tl, ubh, ubl, rhs, points = call(
        prepare_kernel,
        pair(len(inside) * leaf, leaf)
        + pair(leaves, 2 * rank, leaf)
        + [shape(probes, count), shape(EXTRA, count)],
        far_memory(near_list, probe_rhs, coords, leaf_basis, transfer, device),
        scalars=1,
        scratch=[(3, count, LANE)],
        name="prepare",
        flops=4 * 10**9,
    )
    (term,) = call(
        term_kernel, [shape(probes + EXTRA, LANE)], (own, r1, r2, r3), name="term"
    )
    gathered = spread_groups(term)
    hh, hl, klh, kll, part = call(
        border_kernel,
        pair(len(across) * leaf, leaf)
        + pair(lax.axis_size("sub") * span, span)
        + [shape(probes, count)],
        (near_list, far_leaf_list, rhs, own, r1, r2, r3, r4, points, th, tl, ubh, ubl),
        scalars=2,
        scratch=[
            (EXTRA, 2 * half),
            (3, 2 * half, LANE),
            (lax.axis_size("sub"), 3, span, LANE),
        ],
        name="border",
        flops=4 * 10**9,
    )
    image, kgh, kgl, *sent = call(
        middle_kernel,
        [shape(probes, count)] + pair(rank, groups * rank) + messages(probes),
        (part, gathered, ubh, ubl),
        scratch=[(EXTRA, groups * rank), (3, LANE, LANE)],
        name="middle",
    )
    own = sent[1]
    r1, r2, r3, r4 = exchange(*sent)
    dense = groups * rank <= DENSE
    if dense:
        kgh, kgl = call(
            groups_kernel,
            pair(groups * rank, groups * rank),
            (gathered,),
            scratch=[(EXTRA, groups * rank), (3, groups * rank, LANE)],
            name="groups",
            flops=2 * 10**9,
        )
    part, message = call(
        local_kernel,
        [shape(probes, count), shape(probes, LANE)],
        (rhs, image, own, r1, r2, r3, r4, th, tl, hh, hl, klh, kll, ubh, ubl),
        name="local",
    )
    gathered = spread_groups(message)
    sums = jnp.sum(gathered, axis=0)
    shares = [swap(sums, "sub", m) for m in range(1, lax.axis_size("sub"))]
    second, group_pair = call(
        last_kernel,
        [shape(probes, count), shape(probes, LANE)],
        (part, gathered, kgh, kgl, ubh, ubl),
        name="last",
        flops=10**9,
    )
    if not dense:
        group_pair = lax.psum(group_pair, "leaf")
    return call(
        partial(update_kernel, rank),
        [shape(probes, count), shape(probes, count)],
        (sums, *shares, group_pair, rhs, image, second),
        name="update",
    )


def solution(mesh):
    return jax.shard_map(
        shards,
        mesh=mesh,
        in_specs=(
            P(None, ("leaf", "sub")),
            P(None, ("leaf", "sub")),
            P(("leaf", "sub"), None),
            P(("leaf", "sub"), None),
            P("leaf", None),
            P(("leaf", "sub"), None, None),
            P(None, ("leaf", "sub")),
            P(("leaf", "sub"), None, None),
            P(("leaf", "sub"), None, None),
            P(None, "leaf"),
        ),
        out_specs=(P(None, ("leaf", "sub")), P(None, ("leaf", "sub"))),
        check_vma=False,
    )
```

```python
import jax
import jax.numpy as jnp
from jax import lax
from jax.experimental import pallas as pl
from jax.experimental.pallas import tpu as pltpu
from jax.sharding import PartitionSpec as P

REACH = 2
NOISE = 1.0
ROOT_FIVE = 5.0**0.5
LOG2_E = 1.4426950408889634
HIGHEST = lax.Precision.HIGHEST
F32 = jnp.float32
BF16 = jnp.bfloat16
DOWN = 2.0**-40
UP = 2.0**20
LANE = 128
EXTRA = 8
CHUNK = 32
SHARES = 4
GRANT = 16 * 2**20
DENSE = 1024


def dot(a, b, ca=1, cb=0):
    return lax.dot_general(
        a, b, (((ca,), (cb,)), ((), ())), precision=HIGHEST, preferred_element_type=F32
    )


def split(x):
    high = x.astype(BF16)
    return high, (x - high.astype(F32)).astype(BF16)


def stacked(x):
    return jnp.concatenate(split(x), axis=0)


def product(stack, high, low, transposed=False):
    rows = stack.shape[0] // 2
    dims = (((1,), (1 if transposed else 0,)), ((), ()))
    both = lax.dot_general(stack, high, dims, preferred_element_type=F32)
    more = lax.dot_general(stack[:rows], low, dims, preferred_element_type=F32)
    return (both[:rows] + both[rows:]) + more


def matern(rows, cols, weight):
    total = None
    for row, col in zip(rows, cols):
        spread = row - col
        total = spread * spread if total is None else total + spread * spread
    distance = total * lax.rsqrt(jnp.maximum(total, 1e-35))
    poly = (weight + (ROOT_FIVE * weight) * distance) + ((5.0 / 3.0) * weight) * total
    return poly * jnp.exp2((-ROOT_FIVE * LOG2_E) * distance)


def named(list_ref, row, index):
    hit = list_ref[row, 0] == index
    for column in range(1, list_ref.shape[1]):
        hit = jnp.logical_or(hit, list_ref[row, column] == index)
    return jnp.where(hit, 1.0, 0.0).astype(F32)


def padded_lanes(x, lanes):
    return jnp.concatenate(
        [x, jnp.zeros((x.shape[0], lanes - x.shape[1]), x.dtype)], axis=1
    )


def padded_rows(x, rows):
    return jnp.concatenate(
        [x, jnp.zeros((rows - x.shape[0], x.shape[1]), x.dtype)], axis=0
    )


def write_messages(vec, coefs, term, outs, half, rows):
    m1, own, m4 = outs
    count = vec.shape[1]
    even = lax.axis_index("sub") % 2 == 0
    low = vec[:, :half]
    high = vec[:, count - half :]
    span = coefs.shape[1]
    base = own.shape[1]
    for ref in (m1, own):
        ref[rows, 0:span] = coefs
        ref[rows, span:base] = term
    m1[rows, base : base + half] = jnp.where(even, high, low)
    m4[rows, :] = jnp.where(even, low, high)


def halos(r1, r4, rows, base):
    odd = lax.axis_index("sub") % 2 == 1
    from_a = r1[rows, base:]
    from_b = r4[rows, :]
    return jnp.where(odd, from_a, from_b), jnp.where(odd, from_b, from_a)


def first_kernel(
    list_ref, vec_ref, coords_ref, skel_ref, gskel_ref, basis_ref, transfer_ref, device_ref,
    m1_ref, own_ref, m4_ref, rhs_ref, points_ref, basis_out, transfer_out, device_out,
):
    outs = (m1_ref, own_ref, m4_ref)
    leaves, _, leaf = basis_ref.shape
    probes = vec_ref.shape[0]
    half = REACH * leaf
    vec = vec_ref[...]
    coefs = jnp.concatenate(
        [dot(vec[:, i * leaf : (i + 1) * leaf], basis_ref[i], 1, 1) for i in range(leaves)],
        axis=1,
    )
    term = padded_lanes(dot(dot(coefs, transfer_ref[...]), device_ref[...]), LANE)
    write_messages(vec, coefs, term, outs, half, slice(0, probes))
    relative = lax.axis_index("leaf") ^ lax.broadcasted_iota(jnp.int32, (1, LANE), 1)
    listed = jnp.zeros((1, LANE), F32)
    for column in range(list_ref.shape[1]):
        listed = jnp.where(relative == list_ref[0, column], 1.0, listed)
    group_rows = jnp.concatenate([padded_lanes(gskel_ref[...], LANE), listed], axis=0)
    write_messages(
        padded_rows(coords_ref[...], EXTRA),
        padded_rows(skel_ref[...], EXTRA),
        padded_rows(group_rows, EXTRA),
        outs,
        half,
        slice(probes, probes + EXTRA),
    )
    rhs_ref[...] = vec
    points_ref[...] = padded_rows(coords_ref[...], EXTRA)
    basis_out[...] = basis_ref[...]
    transfer_out[...] = transfer_ref[...]
    device_out[...] = device_ref[...]


def spread_columns(points, wide_ref):
    columns = points.T
    for axis in range(3):
        wide_ref[axis] = jnp.broadcast_to(
            columns[:, axis : axis + 1], (columns.shape[0], LANE)
        )


def fill_tile(wide_ref, source, points_ref, top_row, lane, width, weight, pair, row, size):
    high_ref, low_ref = pair

    def body(step, _):
        start = pl.multiple_of(source + step * CHUNK, CHUNK)
        target = pl.multiple_of(row + step * CHUNK, CHUNK)
        rows = [wide_ref[axis, pl.ds(start, CHUNK), :] for axis in range(3)]
        for at in range(0, width, LANE):
            cols = [
                points_ref[top_row + axis : top_row + axis + 1, lane + at : lane + at + LANE]
                for axis in range(3)
            ]
            factor = weight[:, at : at + LANE] if weight.ndim else weight
            top, rest = split(matern(rows, cols, factor))
            high_ref[pl.ds(target, CHUNK), at : at + LANE] = top
            low_ref[pl.ds(target, CHUNK), at : at + LANE] = rest
        return 0

    lax.fori_loop(0, size // CHUNK, body, 0, unroll=2)


def window_tiles(leaves):
    inside = []
    across = []
    for i in range(leaves):
        for j in range(i - REACH, i + REACH + 1):
            if not 0 <= j < leaves:
                across.append((i, j))
            elif j >= i:
                inside.append((i, j))
    return inside, across


def prepare_kernel(
    near_ref, points_ref, basis_ref, transfer_ref, device_ref,
    th_ref, tl_ref, ubh_ref, ubl_ref, wide_ref,
):
    leaves, rank, leaf = basis_ref.shape
    first = (lax.axis_index("leaf") * lax.axis_size("sub") + lax.axis_index("sub")) * leaves
    spread_columns(points_ref[...], wide_ref)
    for at, (i, j) in enumerate(window_tiles(leaves)[0]):
        fill_tile(
            wide_ref, j * leaf, points_ref, 0, i * leaf, leaf, named(near_ref, i, first + j),
            (th_ref, tl_ref), at * leaf, leaf,
        )
    chain = dot(transfer_ref[...], device_ref[...])
    for i in range(leaves):
        basis = basis_ref[i]
        group_basis = dot(chain[i * rank : (i + 1) * rank], basis, 0, 0)
        top, rest = split(jnp.concatenate([basis, group_basis], axis=0))
        ubh_ref[i] = top
        ubl_ref[i] = rest


def folded(x, rank):
    half = x.shape[0] // 2
    return jnp.concatenate([x[:half, :rank], x[half:, :rank]], axis=1)


def summed_terms(own, r1, r2, r3, rows, span):
    lanes = slice(span, span + LANE)
    return (own[rows, lanes] + r1[rows, lanes]) + (r2[rows, lanes] + r3[rows, lanes])


def term_kernel(own, r1, r2, r3, out_ref):
    half = out_ref.shape[0] - EXTRA
    span = own.shape[1] - LANE
    out_ref[half:, :] = own[2 * half :, span:]
    out_ref[0:half, :] = folded(
        summed_terms(own, r1, r2, r3, slice(0, 2 * half), span), LANE // 2
    )


def leaf_slice(x, i, leaf):
    return x[:, i * leaf : (i + 1) * leaf]


def inner_kernel(vec_ref, th_ref, tl_ref, out_ref):
    vec = vec_ref[...]
    leaf = th_ref.shape[1]
    leaves = vec.shape[1] // leaf
    stack = stacked(vec)
    totals = [NOISE * leaf_slice(vec, i, leaf) for i in range(leaves)]
    for at, (i, j) in enumerate(window_tiles(leaves)[0]):
        rows = slice(at * leaf, (at + 1) * leaf)
        high, low = th_ref[rows, :], tl_ref[rows, :]
        totals[i] = totals[i] + product(leaf_slice(stack, j, leaf), high, low)
        if j > i:
            totals[j] = totals[j] + product(leaf_slice(stack, i, leaf), high, low, True)
    out_ref[...] = jnp.concatenate(totals, axis=1)


def local_part(inner_ref, low, high, blocks, tiles, bases, out_ref):
    hh_ref, hl_ref, klh_ref, kll_ref = tiles
    ubh_ref, ubl_ref = bases
    leaves, double, leaf = ubh_ref.shape
    rank = double // 2
    across = window_tiles(leaves)[1]
    low, high = stacked(low), stacked(high)

    def piece(j):
        return leaf_slice(low, j + REACH, leaf) if j < 0 else leaf_slice(high, j - leaves, leaf)

    far = product(stacked(jnp.concatenate(blocks, axis=1)), klh_ref[...], kll_ref[...])
    far_stack = stacked(far)
    near = []
    for i in range(leaves):
        total = inner_ref[:, i * leaf : (i + 1) * leaf]
        at = [n for n, pair in enumerate(across) if pair[0] == i]
        if at:
            where = slice(at[0] * leaf, (at[-1] + 1) * leaf)
            wide = jnp.concatenate([piece(across[n][1]) for n in at], axis=1)
            total = total + product(wide, hh_ref[where, :], hl_ref[where, :])
        near.append(total)
        out_ref[:, i * leaf : (i + 1) * leaf] = total + product(
            far_stack[:, i * rank : (i + 1) * rank], ubh_ref[i, 0:rank, :], ubl_ref[i, 0:rank, :]
        )
    return jnp.concatenate(near, axis=1), far


def skeleton_kernel(far_ref, own, r1, r2, r3, klh_ref, kll_ref, wide_ref):
    leaves = far_ref.shape[0]
    span = klh_ref.shape[1]
    rank = span // leaves
    probes = own.shape[0] - EXTRA
    sub = lax.axis_index("sub")
    group_first = lax.axis_index("leaf") * lax.axis_size("sub") * leaves
    messages = (own, r1, r2, r3)
    lane_leaf = lax.broadcasted_iota(jnp.int32, (1, span), 1) // rank
    for m, message in enumerate(messages):
        spread_columns(message[probes : probes + EXTRA, 0:span], wide_ref.at[m])
    for m in range(len(messages)):
        for j in range(leaves):
            index = group_first + (sub ^ m) * leaves + j
            mask = jnp.zeros((1, span), F32)
            for i in range(leaves):
                mask = jnp.where(lane_leaf == i, named(far_ref, i, index), mask)
            fill_tile(
                wide_ref.at[m], j * rank, own, probes, 0, span, mask,
                (klh_ref, kll_ref), m * span + j * rank, rank,
            )


def border_kernel(near_ref, r1, r4, points_ref, hh_ref, hl_ref, ends_ref, wide_ref):
    leaves = near_ref.shape[0]
    count = points_ref.shape[1]
    leaf = count // leaves
    half = REACH * leaf
    probes = r4.shape[0] - EXTRA
    first = (lax.axis_index("leaf") * lax.axis_size("sub") + lax.axis_index("sub")) * leaves
    low, high = halos(r1, r4, slice(probes, probes + EXTRA), r1.shape[1] - half)
    ends_ref[:, 0:half] = low
    ends_ref[:, half:] = high
    spread_columns(ends_ref[...], wide_ref)
    for at, (i, j) in enumerate(window_tiles(leaves)[1]):
        source = (j + REACH) * leaf if j < 0 else half + (j - leaves) * leaf
        fill_tile(
            wide_ref, source, points_ref, 0, i * leaf, leaf, named(near_ref, i, first + j),
            (hh_ref, hl_ref), at * leaf, leaf,
        )


def outer_kernel(
    inner_ref, own, r1, r2, r3, r4, hh_ref, hl_ref, klh_ref, kll_ref, ubh_ref, ubl_ref, part_ref,
):
    span = klh_ref.shape[1]
    rows = slice(0, inner_ref.shape[0])
    low, high = halos(r1, r4, rows, own.shape[1])
    local_part(
        inner_ref, low, high, [r[rows, 0:span] for r in (own, r1, r2, r3)],
        (hh_ref, hl_ref, klh_ref, kll_ref), (ubh_ref, ubl_ref), part_ref,
    )


def row_sum(x):
    return jnp.sum(x, axis=1, keepdims=True)


def local_kernel(
    rhs_ref, vec_ref, inner_ref, own, r1, r2, r3, r4, hh_ref, hl_ref, klh_ref, kll_ref,
    ubh_ref, ubl_ref, part_ref, message_ref,
):
    base = own.shape[1]
    span = klh_ref.shape[1]
    rank = ubh_ref.shape[1] // 2
    rows = slice(0, vec_ref.shape[0])
    rhs = rhs_ref[...]
    vec = vec_ref[...]
    low, high = halos(r1, r4, rows, base)
    blocks = [r[rows, 0:span] for r in (own, r1, r2, r3)]
    near, far = local_part(
        inner_ref, low, high, blocks,
        (hh_ref, hl_ref, klh_ref, kll_ref), (ubh_ref, ubl_ref), part_ref,
    )
    shares = (
        row_sum(rhs * rhs),
        row_sum(rhs * vec),
        row_sum(vec * vec),
        row_sum((DOWN * vec) * near) + row_sum((DOWN * blocks[0]) * far),
    )
    lane = lax.broadcasted_iota(jnp.int32, (vec.shape[0], LANE), 1)
    columns = jnp.zeros((vec.shape[0], LANE), F32)
    for at, share in enumerate(shares):
        columns = jnp.where(lane == at, share, columns)
    term = folded(summed_terms(own, r1, r2, r3, rows, span), rank)
    size = term.shape[0] // lax.axis_size("sub")
    sub = lax.axis_index("sub")
    mine = term[0:size]
    for m in range(1, lax.axis_size("sub")):
        mine = jnp.where(sub == m, term[m * size : (m + 1) * size], mine)
    message = jnp.concatenate([mine, padded_lanes(columns.T[0:SHARES], LANE)], axis=0)
    for m in range(message_ref.shape[0]):
        message_ref[m] = message


def exchange_order(groups):
    order = [0]
    for offsets in exchange_rounds(groups):
        order = order + [m ^ offset for offset in offsets for m in order]
    return order


def exchange_rounds(groups):
    if groups == 8:
        return [[2, 4, 6], [1]]
    return [[groups >> n] for n in range(1, groups.bit_length())]


def group_points(group_ref, half, rank):
    groups = group_ref.shape[0]
    return jnp.concatenate(
        [group_ref[m, half : half + EXTRA, 0:rank] for m in range(groups)], axis=1
    )


def group_row(group_ref, half, rank, places):
    return jnp.concatenate(
        [
            jnp.concatenate(
                [group_ref[m, 0:half, at : at + rank] for m in places], axis=1
            )
            for at in (0, rank)
        ],
        axis=0,
    )


def group_mask(group_ref, row, block, rank):
    groups = group_ref.shape[0]
    order = exchange_order(groups)
    listed = group_ref[block, row : row + 1, :]
    lane_group = lax.broadcasted_iota(jnp.int32, (1, groups * rank), 1) // rank
    mask = jnp.zeros((1, groups * rank), F32)
    for m in range(groups):
        at = order[block] ^ order[m]
        mask = jnp.where(lane_group == m, listed[:, at : at + 1], mask)
    return mask


def middle_kernel(
    part_ref, group_ref, ubh_ref, ubl_ref, image_ref, kgh_ref, kgl_ref, *rest,
):
    outs = rest[:3]
    points_ref, wide_ref = rest[3:]
    leaves, double, leaf = ubh_ref.shape
    rank = double // 2
    groups = group_ref.shape[0]
    probes = part_ref.shape[0]
    half = probes // 2
    points_ref[...] = group_points(group_ref, half, rank)
    spread_columns(group_ref[0, half : half + EXTRA, :], wide_ref)
    fill_tile(
        wide_ref, 0, points_ref, 0, 0, groups * rank,
        group_mask(group_ref, half + 3, 0, rank), (kgh_ref, kgl_ref), 0, rank,
    )
    held = group_row(group_ref, half, rank, range(groups))
    group_far = product(stacked(held), kgh_ref[...], kgl_ref[...], True)
    group_stack = stacked(group_far)
    image = []
    coefs = []
    term = None
    for i in range(leaves):
        piece = part_ref[:, i * leaf : (i + 1) * leaf] + product(
            group_stack, ubh_ref[i, rank:, :], ubl_ref[i, rank:, :]
        )
        image.append(piece)
        both = product(stacked(piece), ubh_ref[i], ubl_ref[i], True)
        coefs.append(both[:, :rank])
        term = both if term is None else term + both
    image = jnp.concatenate(image, axis=1)
    image_ref[...] = image
    write_messages(
        image, jnp.concatenate(coefs, axis=1), padded_lanes(term[:, rank:], LANE), outs,
        REACH * leaf, slice(0, probes),
    )


def groups_kernel(group_ref, kah_ref, kal_ref, points_ref, wide_ref):
    groups, rows, _ = group_ref.shape
    rank = kah_ref.shape[0] // groups
    half = rows - EXTRA
    points_ref[...] = group_points(group_ref, half, rank)
    spread_columns(points_ref[...], wide_ref)
    for m in range(groups):
        fill_tile(
            wide_ref, m * rank, points_ref, 0, 0, groups * rank,
            group_mask(group_ref, half + 3, m, rank), (kah_ref, kal_ref), m * rank, rank,
        )


def second_image(part_ref, group_ref, kah_ref, kal_ref, ubh_ref, ubl_ref):
    leaves, double, leaf = ubh_ref.shape
    rank = double // 2
    subs = lax.axis_size("sub")
    size = group_ref.shape[1] - SHARES
    mine = lax.axis_index("leaf")
    pieces = []
    for m in exchange_order(group_ref.shape[0] // subs):
        at = (mine ^ m) * subs
        pieces.append(jnp.concatenate([group_ref[at + k, 0:size, :] for k in range(subs)], axis=0))
    held = jnp.concatenate(
        [
            jnp.concatenate([x[:, lane : lane + rank] for x in pieces], axis=1)
            for lane in (0, rank)
        ],
        axis=0,
    )
    far = product(stacked(held), kah_ref[...], kal_ref[...], True)
    group_stack = stacked(far[:, :rank])
    second = [
        part_ref[:, i * leaf : (i + 1) * leaf]
        + product(group_stack, ubh_ref[i, rank:, :], ubl_ref[i, rank:, :])
        for i in range(leaves)
    ]
    return second, row_sum((DOWN * held[:, : far.shape[1]]) * far)


def update(group_ref, share, vec_ref, first_ref, second, solution_ref, residual_ref):
    total = group_ref[0]
    for q in range(1, group_ref.shape[0]):
        total = total + group_ref[q]
    sums = total.T[0 : vec_ref.shape[0]]
    at = group_ref.shape[1] - SHARES
    bb, bw, ww, wv = (sums[:, at + k : at + k + 1] for k in range(SHARES))
    wv = wv + share
    step = bb / bw
    rise = (step * ww) * step
    norm = rise - bb
    grow = rise / bb
    scaled = step * UP
    curvature = (grow * grow) * bw - (2.0 * grow) * (step * ww) + (scaled * wv) * scaled
    again = norm / curvature
    leaf = second[0].shape[1]
    for i, image in enumerate(second):
        lanes = slice(i * leaf, (i + 1) * leaf)
        vec = vec_ref[:, lanes]
        first = first_ref[:, lanes]
        direction = grow * vec - step * first
        solution_ref[:, lanes] = step * vec + again * direction
        residual_ref[:, lanes] = (vec - step * first) - again * (grow * first - step * image)


def final_kernel(
    part_ref, group_ref, kah_ref, kal_ref, ubh_ref, ubl_ref, vec_ref, first_ref,
    solution_ref, residual_ref,
):
    second, share = second_image(part_ref, group_ref, kah_ref, kal_ref, ubh_ref, ubl_ref)
    update(group_ref, share, vec_ref, first_ref, second, solution_ref, residual_ref)


def last_kernel(part_ref, group_ref, kah_ref, kal_ref, ubh_ref, ubl_ref, second_ref, share_ref):
    second, share = second_image(part_ref, group_ref, kah_ref, kal_ref, ubh_ref, ubl_ref)
    second_ref[...] = jnp.concatenate(second, axis=1)
    share_ref[...] = jnp.broadcast_to(share, share_ref.shape)


def update_kernel(
    group_ref, share_ref, vec_ref, first_ref, second_ref, solution_ref, residual_ref
):
    update(
        group_ref, share_ref[:, 0:1], vec_ref, first_ref, [second_ref[...]],
        solution_ref, residual_ref,
    )


def vmem(count):
    return [pl.BlockSpec(memory_space=pltpu.VMEM)] * count


def smem(count):
    return [pl.BlockSpec(memory_space=pltpu.SMEM)] * count


def shape(*dims, dtype=F32):
    return jax.ShapeDtypeStruct(dims, dtype)


def pair(*dims):
    return [shape(*dims, dtype=BF16)] * 2


def call(kernel, outs, args, scalars=0, scratch=(), flops=0):
    return pl.pallas_call(
        kernel,
        out_shape=tuple(outs),
        in_specs=smem(scalars) + vmem(len(args) - scalars),
        out_specs=tuple(vmem(len(outs))),
        scratch_shapes=[pltpu.VMEM(dims, F32) for dims in scratch],
        compiler_params=pltpu.CompilerParams(vmem_limit_bytes=GRANT),
        cost_estimate=pl.CostEstimate(
            flops=flops, transcendentals=0, bytes_accessed=1000000
        ),
    )(*args)


def swap(x, axis, m):
    return lax.ppermute(x, axis, [(i, i ^ m) for i in range(lax.axis_size(axis))])


def exchange(m1, own, m4):
    nodes = lax.axis_size("sub") * lax.axis_size("leaf")
    across = [(q, q + 1) for q in range(1, nodes - 1, 2)]
    across = across + [(target, source) for source, target in across]
    received = swap(m1, "sub", 1), swap(own, "sub", 2), swap(own, "sub", 3)
    return *received, lax.ppermute(m4, ("leaf", "sub"), across)


def spread_groups(held):
    held = held[None]
    for offsets in exchange_rounds(lax.axis_size("leaf")):
        held = jnp.concatenate([held] + [swap(held, "leaf", offset) for offset in offsets], axis=0)
    return held


def far_memory(*args):
    return [pltpu.with_memory_space_constraint(x, pltpu.HBM) for x in args]


def shards(
    probe_rhs,
    coords,
    near_list,
    far_leaf_list,
    far_group_list,
    leaf_basis,
    leaf_skeleton,
    leaf_transfer,
    device_transfer,
    group_skeleton,
):
    leaves, rank, leaf = leaf_basis.shape
    probes, count = probe_rhs.shape
    groups = lax.axis_size("leaf")
    subs = lax.axis_size("sub")
    half = REACH * leaf
    span = leaves * rank
    base = span + LANE
    inside, across = window_tiles(leaves)
    transfer = leaf_transfer.reshape(span, rank)
    device = device_transfer[0]

    def messages(rows):
        return [shape(rows, base + half), shape(rows, base), shape(rows, half)]

    *sent, rhs, points, basis, transfer, device = call(
        first_kernel,
        messages(probes + EXTRA)
        + [
            shape(probes, count),
            shape(EXTRA, count),
            shape(leaves, rank, leaf),
            shape(span, rank),
            shape(rank, rank),
        ],
        far_memory(
            far_group_list, probe_rhs, coords, leaf_skeleton, group_skeleton, leaf_basis,
            transfer, device,
        ),
        scalars=1,
    )
    own = sent[1]
    r1, r2, r3, r4 = exchange(*sent)
    th, tl, ubh, ubl = call(
        prepare_kernel,
        pair(len(inside) * leaf, leaf)
        + pair(leaves, 2 * rank, leaf),
        (near_list, points, basis, transfer, device),
        scalars=1,
        scratch=[(3, count, LANE)],
    )
    (term,) = call(term_kernel, [shape(probes // 2 + EXTRA, LANE)], (own, r1, r2, r3))
    gathered = spread_groups(term)
    klh, kll = call(
        skeleton_kernel,
        pair(subs * span, span),
        (far_leaf_list, own, r1, r2, r3),
        scalars=1,
        scratch=[(subs, 3, span, LANE)],
    )
    hh, hl = call(
        border_kernel,
        pair(len(across) * leaf, leaf),
        (near_list, r1, r4, points),
        scalars=1,
        scratch=[(EXTRA, 2 * half), (3, 2 * half, LANE)],
    )
    (inner,) = call(inner_kernel, [shape(probes, count)], (rhs, th, tl))
    (part,) = call(
        outer_kernel,
        [shape(probes, count)],
        (inner, own, r1, r2, r3, r4, hh, hl, klh, kll, ubh, ubl),
    )
    image, kgh, kgl, *sent = call(
        middle_kernel,
        [shape(probes, count)] + pair(rank, groups * rank) + messages(probes),
        (part, gathered, ubh, ubl),
        scratch=[(EXTRA, groups * rank), (3, LANE, LANE)],
    )
    own = sent[1]
    r1, r2, r3, r4 = exchange(*sent)
    dense = groups * rank <= DENSE
    if dense:
        kgh, kgl = call(
            groups_kernel,
            pair(groups * rank, groups * rank),
            (gathered,),
            scratch=[(EXTRA, groups * rank), (3, groups * rank, LANE)],
        )
    (inner,) = call(inner_kernel, [shape(probes, count)], (image, th, tl))
    part, message = call(
        local_kernel,
        [
            shape(probes, count),
            shape(groups * subs, probes // 2 // subs + SHARES, LANE),
        ],
        (rhs, image, inner, own, r1, r2, r3, r4, hh, hl, klh, kll, ubh, ubl),
    )
    gathered = lax.all_to_all(message, ("leaf", "sub"), 0, 0)
    outs = [shape(probes, count), shape(probes, count)]
    if dense:
        return call(final_kernel, outs, (part, gathered, kgh, kgl, ubh, ubl, rhs, image))
    second, share = call(
        last_kernel,
        [shape(probes, count), shape(probes, LANE)],
        (part, gathered, kgh, kgl, ubh, ubl),
    )
    share = lax.psum(share, "leaf")
    return call(update_kernel, outs, (gathered, share, rhs, image, second))


def solution(mesh):
    return jax.shard_map(
        shards,
        mesh=mesh,
        in_specs=(
            P(None, ("leaf", "sub")),
            P(None, ("leaf", "sub")),
            P(("leaf", "sub"), None),
            P(("leaf", "sub"), None),
            P("leaf", None),
            P(("leaf", "sub"), None, None),
            P(None, ("leaf", "sub")),
            P(("leaf", "sub"), None, None),
            P(("leaf", "sub"), None, None),
            P(None, "leaf"),
        ),
        out_specs=(P(None, ("leaf", "sub")), P(None, ("leaf", "sub"))),
        check_vma=False,
    )
```

```python
import jax
import jax.numpy as jnp
from jax import lax
from jax.experimental import pallas as pl
from jax.experimental.pallas import tpu as pltpu
from jax.sharding import PartitionSpec as P

REACH = 2
NOISE = 1.0
ROOT_FIVE = 5.0**0.5
LOG2_E = 1.4426950408889634
HIGHEST = lax.Precision.HIGHEST
F32 = jnp.float32
BF16 = jnp.bfloat16
DOWN = 2.0**-40
UP = 2.0**20
LANE = 128
EXTRA = 8
CHUNK = 32
UNROLL = 1024
SHARES = 4
GRANT = 16 * 2**20
DENSE = 1024


def dot(a, b, ca=1, cb=0):
    return lax.dot_general(
        a, b, (((ca,), (cb,)), ((), ())), precision=HIGHEST, preferred_element_type=F32
    )


def split(x):
    high = x.astype(BF16)
    return high, (x - high.astype(F32)).astype(BF16)


def stacked(x):
    return jnp.concatenate(split(x), axis=0)


def product(stack, high, low, transposed=False):
    rows = stack.shape[0] // 2
    dims = (((1,), (1 if transposed else 0,)), ((), ()))
    both = lax.dot_general(stack, high, dims, preferred_element_type=F32)
    more = lax.dot_general(stack[:rows], low, dims, preferred_element_type=F32)
    return (both[:rows] + both[rows:]) + more


def matern(rows, cols, weight):
    total = None
    for row, col in zip(rows, cols):
        spread = row - col
        total = spread * spread if total is None else total + spread * spread
    distance = total * lax.rsqrt(jnp.maximum(total, 1e-35))
    poly = (weight + (ROOT_FIVE * weight) * distance) + ((5.0 / 3.0) * weight) * total
    return poly * jnp.exp2((-ROOT_FIVE * LOG2_E) * distance)


def slot_columns(list_ref):
    leaves, slots = list_ref.shape
    block = jnp.full((EXTRA, LANE), -2, jnp.int32)
    tall = jnp.concatenate([list_ref[...], block[leaves:, 0:slots]], axis=0)
    wide = jnp.concatenate([tall, block[:, 0 : LANE - slots]], axis=1)
    return wide.T[0 : -(-slots // EXTRA) * EXTRA]


def named(columns, index):
    return jnp.max(jnp.where(columns == index, 1.0, 0.0).astype(F32), axis=0, keepdims=True)


def padded_lanes(x, lanes):
    return jnp.concatenate(
        [x, jnp.zeros((x.shape[0], lanes - x.shape[1]), x.dtype)], axis=1
    )


def padded_rows(x, rows):
    return jnp.concatenate(
        [x, jnp.zeros((rows - x.shape[0], x.shape[1]), x.dtype)], axis=0
    )


def ends(vec, half):
    even = lax.axis_index("sub") % 2 == 0
    low = vec[:, :half]
    high = vec[:, vec.shape[1] - half :]
    return jnp.where(even, high, low), jnp.where(even, low, high)


def write_row(ref, rows, *pieces):
    at = 0
    for piece in pieces:
        ref[rows, at : at + piece.shape[1]] = piece
        at = at + piece.shape[1]


def halos(r1, from_b, rows, base):
    odd = lax.axis_index("sub") % 2 == 1
    from_a = r1[rows, base:]
    return jnp.where(odd, from_a, from_b), jnp.where(odd, from_b, from_a)


def first_kernel(
    list_ref, vec_ref, coords_ref, skel_ref, gskel_ref, basis_ref, transfer_ref, device_ref,
    near_ref, far_ref,
    m1_ref, own_ref, m4_ref, rhs_ref, points_ref, basis_out, transfer_out, device_out,
    near_out, far_out,
):
    leaves, _, leaf = basis_ref.shape
    probes = vec_ref.shape[0]
    half = REACH * leaf
    vec = vec_ref[...]
    coefs = jnp.concatenate(
        [dot(vec[:, i * leaf : (i + 1) * leaf], basis_ref[i], 1, 1) for i in range(leaves)],
        axis=1,
    )
    term = padded_lanes(dot(dot(coefs, transfer_ref[...]), device_ref[...]), LANE)
    relative = lax.axis_index("leaf") ^ lax.broadcasted_iota(jnp.int32, (1, LANE), 1)
    listed = jnp.zeros((1, LANE), F32)
    for column in range(list_ref.shape[1]):
        listed = jnp.where(relative == list_ref[0, column], 1.0, listed)
    group_rows = jnp.concatenate([padded_lanes(gskel_ref[...], LANE), listed], axis=0)
    points = padded_rows(coords_ref[...], EXTRA)
    skel = padded_rows(skel_ref[...], EXTRA)
    group_rows = padded_rows(group_rows, EXTRA)
    for rows, block in (
        (slice(0, probes), (vec, coefs, term)),
        (slice(probes, probes + EXTRA), (points, skel, group_rows)),
    ):
        part_a, part_b = ends(block[0], half)
        write_row(m1_ref, rows, *block[1:], part_a)
        write_row(own_ref, rows, *block[1:])
        write_row(m4_ref, rows, part_b)
    rhs_ref[...] = vec
    points_ref[...] = points
    basis_out[...] = basis_ref[...]
    transfer_out[...] = transfer_ref[...]
    device_out[...] = device_ref[...]
    near_out[...] = near_ref[...]
    far_out[...] = far_ref[...]


def spread_columns(points, wide_ref):
    columns = points.T
    for axis in range(3):
        wide_ref[axis] = jnp.broadcast_to(
            columns[:, axis : axis + 1], (columns.shape[0], LANE)
        )


def fill_tile(wide_ref, source, points_ref, top_row, lane, width, weight, pair, row, size):
    high_ref, low_ref = pair

    def body(step, _):
        start = pl.multiple_of(source + step * CHUNK, CHUNK)
        target = pl.multiple_of(row + step * CHUNK, CHUNK)
        rows = [wide_ref[axis, pl.ds(start, CHUNK), :] for axis in range(3)]
        for at in range(0, width, LANE):
            cols = [
                points_ref[top_row + axis : top_row + axis + 1, lane + at : lane + at + LANE]
                for axis in range(3)
            ]
            factor = weight if weight.shape[1] == LANE else weight[:, at : at + LANE]
            top, rest = split(matern(rows, cols, factor))
            high_ref[pl.ds(target, CHUNK), at : at + LANE] = top
            low_ref[pl.ds(target, CHUNK), at : at + LANE] = rest
        return 0

    lax.fori_loop(0, size // CHUNK, body, 0, unroll=min(size // CHUNK, UNROLL // width))


def window_tiles(leaves):
    inside = []
    across = []
    for i in range(leaves):
        for j in range(i - REACH, i + REACH + 1):
            if not 0 <= j < leaves:
                across.append((i, j))
            elif j >= i:
                inside.append((i, j))
    return inside, across


def prepare_kernel(
    near_ref, points_ref, th_ref, tl_ref, wide_ref,
):
    leaves = near_ref.shape[0]
    leaf = points_ref.shape[1] // leaves
    first = (lax.axis_index("leaf") * lax.axis_size("sub") + lax.axis_index("sub")) * leaves
    spread_columns(points_ref[...], wide_ref)
    slots = slot_columns(near_ref)
    for at, (i, j) in enumerate(window_tiles(leaves)[0]):
        listed = jnp.broadcast_to(slots[:, i : i + 1], (slots.shape[0], LANE))
        fill_tile(
            wide_ref, j * leaf, points_ref, 0, i * leaf, leaf, named(listed, first + j),
            (th_ref, tl_ref), at * leaf, leaf,
        )


def bases_kernel(basis_ref, transfer_ref, device_ref, ubh_ref, ubl_ref):
    leaves, rank, _ = basis_ref.shape
    chain = dot(transfer_ref[...], device_ref[...])
    for i in range(leaves):
        basis = basis_ref[i]
        group_basis = dot(chain[i * rank : (i + 1) * rank], basis, 0, 0)
        top, rest = split(jnp.concatenate([basis, group_basis], axis=0))
        ubh_ref[i] = top
        ubl_ref[i] = rest


def folded(x, rank):
    half = x.shape[0] // 2
    return jnp.concatenate([x[:half, :rank], x[half:, :rank]], axis=1)


def summed_terms(own, r1, r2, r3, rows, span):
    lanes = slice(span, span + LANE)
    return (own[rows, lanes] + r1[rows, lanes]) + (r2[rows, lanes] + r3[rows, lanes])


def term_kernel(own, r1, r2, r3, out_ref):
    half = out_ref.shape[0] - EXTRA
    span = own.shape[1] - LANE
    out_ref[half:, :] = own[2 * half :, span:]
    out_ref[0:half, :] = folded(
        summed_terms(own, r1, r2, r3, slice(0, 2 * half), span), LANE // 2
    )


def leaf_slice(x, i, leaf):
    return x[:, i * leaf : (i + 1) * leaf]


def inner_kernel(vec_ref, th_ref, tl_ref, out_ref):
    vec = vec_ref[...]
    leaf = th_ref.shape[1]
    leaves = vec.shape[1] // leaf
    stack = stacked(vec)
    totals = [NOISE * leaf_slice(vec, i, leaf) for i in range(leaves)]
    for at, (i, j) in enumerate(window_tiles(leaves)[0]):
        rows = slice(at * leaf, (at + 1) * leaf)
        high, low = th_ref[rows, :], tl_ref[rows, :]
        totals[i] = totals[i] + product(leaf_slice(stack, j, leaf), high, low)
        if j > i:
            totals[j] = totals[j] + product(leaf_slice(stack, i, leaf), high, low, True)
    out_ref[...] = jnp.concatenate(totals, axis=1)


def local_part(inner_ref, low, high, blocks, tiles, bases, out_ref):
    hh_ref, hl_ref, klh_ref, kll_ref = tiles
    ubh_ref, ubl_ref = bases
    leaves, double, leaf = ubh_ref.shape
    rank = double // 2
    across = window_tiles(leaves)[1]
    low, high = stacked(low), stacked(high)

    def piece(j):
        return leaf_slice(low, j + REACH, leaf) if j < 0 else leaf_slice(high, j - leaves, leaf)

    far = product(stacked(jnp.concatenate(blocks, axis=1)), klh_ref[...], kll_ref[...])
    far_stack = stacked(far)
    near = []
    for i in range(leaves):
        total = inner_ref[:, i * leaf : (i + 1) * leaf]
        at = [n for n, pair in enumerate(across) if pair[0] == i]
        if at:
            where = slice(at[0] * leaf, (at[-1] + 1) * leaf)
            wide = jnp.concatenate([piece(across[n][1]) for n in at], axis=1)
            total = total + product(wide, hh_ref[where, :], hl_ref[where, :])
        near.append(total)
        out_ref[:, i * leaf : (i + 1) * leaf] = total + product(
            far_stack[:, i * rank : (i + 1) * rank], ubh_ref[i, 0:rank, :], ubl_ref[i, 0:rank, :]
        )
    return jnp.concatenate(near, axis=1), far


def skeleton_kernel(far_ref, own, r1, r2, r3, klh_ref, kll_ref, wide_ref):
    leaves = far_ref.shape[0]
    span = klh_ref.shape[1]
    rank = span // leaves
    probes = own.shape[0] - EXTRA
    sub = lax.axis_index("sub")
    group_first = lax.axis_index("leaf") * lax.axis_size("sub") * leaves
    messages = (own, r1, r2, r3)
    slots = slot_columns(far_ref)
    listed = jnp.concatenate(
        [jnp.broadcast_to(slots[:, i : i + 1], (slots.shape[0], rank)) for i in range(leaves)],
        axis=1,
    )
    for m, message in enumerate(messages):
        spread_columns(message[probes : probes + EXTRA, 0:span], wide_ref.at[m])
    for m in range(len(messages)):
        for j in range(leaves):
            index = group_first + (sub ^ m) * leaves + j
            fill_tile(
                wide_ref.at[m], j * rank, own, probes, 0, span, named(listed, index),
                (klh_ref, kll_ref), m * span + j * rank, rank,
            )


def border_kernel(near_ref, r1, r4, points_ref, hh_ref, hl_ref, ends_ref, wide_ref):
    leaves = near_ref.shape[0]
    count = points_ref.shape[1]
    leaf = count // leaves
    half = REACH * leaf
    probes = r4.shape[0] - EXTRA
    first = (lax.axis_index("leaf") * lax.axis_size("sub") + lax.axis_index("sub")) * leaves
    rows = slice(probes, probes + EXTRA)
    low, high = halos(r1, r4[rows, :], rows, r1.shape[1] - half)
    ends_ref[:, 0:half] = low
    ends_ref[:, half:] = high
    spread_columns(ends_ref[...], wide_ref)
    slots = slot_columns(near_ref)
    for at, (i, j) in enumerate(window_tiles(leaves)[1]):
        listed = jnp.broadcast_to(slots[:, i : i + 1], (slots.shape[0], LANE))
        source = (j + REACH) * leaf if j < 0 else half + (j - leaves) * leaf
        fill_tile(
            wide_ref, source, points_ref, 0, i * leaf, leaf, named(listed, first + j),
            (hh_ref, hl_ref), at * leaf, leaf,
        )


def outer_kernel(
    inner_ref, own, r1, r2, r3, r4, hh_ref, hl_ref, klh_ref, kll_ref, ubh_ref, ubl_ref,
    part_ref,
):
    span = klh_ref.shape[1]
    rows = slice(0, inner_ref.shape[0])
    low, high = halos(r1, r4[rows, :], rows, own.shape[1])
    local_part(
        inner_ref, low, high, [r[rows, 0:span] for r in (own, r1, r2, r3)],
        (hh_ref, hl_ref, klh_ref, kll_ref), (ubh_ref, ubl_ref), part_ref,
    )


def row_sum(x):
    return jnp.sum(x, axis=1, keepdims=True)


def local_kernel(
    rhs_ref, vec_ref, inner_ref, own, r1, r2, r3, r4, hh_ref, hl_ref, klh_ref, kll_ref,
    ubh_ref, ubl_ref, part_ref, message_ref,
):
    base = own.shape[1]
    span = klh_ref.shape[1]
    rank = ubh_ref.shape[1] // 2
    rows = slice(0, vec_ref.shape[0])
    rhs = rhs_ref[...]
    vec = vec_ref[...]
    low, high = halos(r1, r4[...], rows, base)
    blocks = [r[rows, 0:span] for r in (own, r1, r2, r3)]
    near, far = local_part(
        inner_ref, low, high, blocks,
        (hh_ref, hl_ref, klh_ref, kll_ref), (ubh_ref, ubl_ref), part_ref,
    )
    shares = (
        row_sum(rhs * rhs),
        row_sum(rhs * vec),
        row_sum(vec * vec),
        row_sum((DOWN * vec) * near) + row_sum((DOWN * blocks[0]) * far),
    )
    lane = lax.broadcasted_iota(jnp.int32, (vec.shape[0], LANE), 1)
    columns = jnp.zeros((vec.shape[0], LANE), F32)
    for at, share in enumerate(shares):
        columns = jnp.where(lane == at, share, columns)
    term = folded(summed_terms(own, r1, r2, r3, rows, span), rank)
    size = term.shape[0] // lax.axis_size("sub")
    sub = lax.axis_index("sub")
    mine = term[0:size]
    for m in range(1, lax.axis_size("sub")):
        mine = jnp.where(sub == m, term[m * size : (m + 1) * size], mine)
    message = jnp.concatenate([mine, padded_lanes(columns.T[0:SHARES], LANE)], axis=0)
    for m in range(message_ref.shape[0]):
        message_ref[m] = message


def exchange_order(groups):
    order = [0]
    for offsets in exchange_rounds(groups):
        order = order + [m ^ offset for offset in offsets for m in order]
    return order


def exchange_rounds(groups):
    return [[groups >> n] for n in range(1, groups.bit_length())]


def group_points(group_ref, half, rank):
    groups = group_ref.shape[0]
    return jnp.concatenate(
        [group_ref[m, half : half + EXTRA, 0:rank] for m in range(groups)], axis=1
    )


def group_row(group_ref, half, rank, places):
    return jnp.concatenate(
        [
            jnp.concatenate(
                [group_ref[m, 0:half, at : at + rank] for m in places], axis=1
            )
            for at in (0, rank)
        ],
        axis=0,
    )


def group_mask(group_ref, row, block, rank):
    groups = group_ref.shape[0]
    order = exchange_order(groups)
    listed = group_ref[block, row : row + 1, :]
    lane_group = lax.broadcasted_iota(jnp.int32, (1, groups * rank), 1) // rank
    mask = jnp.zeros((1, groups * rank), F32)
    for m in range(groups):
        at = order[block] ^ order[m]
        mask = jnp.where(lane_group == m, listed[:, at : at + 1], mask)
    return mask


def middle_kernel(
    part_ref, group_ref, ubh_ref, ubl_ref, image_ref, kgh_ref, kgl_ref, m4_ref,
    points_ref, wide_ref,
):
    leaves, double, leaf = ubh_ref.shape
    rank = double // 2
    groups = group_ref.shape[0]
    half = part_ref.shape[0] // 2
    points_ref[...] = group_points(group_ref, half, rank)
    spread_columns(group_ref[0, half : half + EXTRA, :], wide_ref)
    fill_tile(
        wide_ref, 0, points_ref, 0, 0, groups * rank,
        group_mask(group_ref, half + 3, 0, rank), (kgh_ref, kgl_ref), 0, rank,
    )
    held = group_row(group_ref, half, rank, range(groups))
    group_far = product(stacked(held), kgh_ref[...], kgl_ref[...], True)
    group_stack = stacked(group_far)
    image = jnp.concatenate(
        [
            part_ref[:, i * leaf : (i + 1) * leaf]
            + product(group_stack, ubh_ref[i, rank:, :], ubl_ref[i, rank:, :])
            for i in range(leaves)
        ],
        axis=1,
    )
    image_ref[...] = image
    m4_ref[...] = ends(image, m4_ref.shape[1])[1]


def second_kernel(vec_ref, ubh_ref, ubl_ref, m1_ref, own_ref):
    leaves, double, leaf = ubh_ref.shape
    rank = double // 2
    vec = vec_ref[...]
    coefs = []
    term = None
    for i in range(leaves):
        both = product(stacked(leaf_slice(vec, i, leaf)), ubh_ref[i], ubl_ref[i], True)
        coefs.append(both[:, :rank])
        term = both if term is None else term + both
    pieces = jnp.concatenate(coefs, axis=1), padded_lanes(term[:, rank:], LANE)
    rows = slice(0, vec.shape[0])
    write_row(own_ref, rows, *pieces)
    write_row(m1_ref, rows, *pieces, ends(vec, REACH * leaf)[0])


def groups_kernel(group_ref, kah_ref, kal_ref, points_ref, wide_ref):
    groups, rows, _ = group_ref.shape
    rank = kah_ref.shape[0] // groups
    half = rows - EXTRA
    points_ref[...] = group_points(group_ref, half, rank)
    spread_columns(points_ref[...], wide_ref)
    for m in range(groups):
        fill_tile(
            wide_ref, m * rank, points_ref, 0, 0, groups * rank,
            group_mask(group_ref, half + 3, m, rank), (kah_ref, kal_ref), m * rank, rank,
        )


def second_image(part_ref, group_ref, kah_ref, kal_ref, ubh_ref, ubl_ref):
    leaves, double, leaf = ubh_ref.shape
    rank = double // 2
    subs = lax.axis_size("sub")
    size = group_ref.shape[1] - SHARES
    mine = lax.axis_index("leaf")
    pieces = []
    for m in exchange_order(group_ref.shape[0] // subs):
        at = (mine ^ m) * subs
        pieces.append(jnp.concatenate([group_ref[at + k, 0:size, :] for k in range(subs)], axis=0))
    held = jnp.concatenate(
        [
            jnp.concatenate([x[:, lane : lane + rank] for x in pieces], axis=1)
            for lane in (0, rank)
        ],
        axis=0,
    )
    far = product(stacked(held), kah_ref[...], kal_ref[...], True)
    group_stack = stacked(far[:, :rank])
    second = [
        part_ref[:, i * leaf : (i + 1) * leaf]
        + product(group_stack, ubh_ref[i, rank:, :], ubl_ref[i, rank:, :])
        for i in range(leaves)
    ]
    return second, row_sum((DOWN * held[:, : far.shape[1]]) * far)


def update(group_ref, share, vec_ref, first_ref, second, solution_ref, residual_ref):
    total = group_ref[0]
    for q in range(1, group_ref.shape[0]):
        total = total + group_ref[q]
    sums = total.T[0 : vec_ref.shape[0]]
    at = group_ref.shape[1] - SHARES
    bb, bw, ww, wv = (sums[:, at + k : at + k + 1] for k in range(SHARES))
    wv = wv + share
    step = bb / bw
    rise = (step * ww) * step
    norm = rise - bb
    grow = rise / bb
    scaled = step * UP
    curvature = (grow * grow) * bw - (2.0 * grow) * (step * ww) + (scaled * wv) * scaled
    again = norm / curvature
    leaf = second[0].shape[1]
    for i, image in enumerate(second):
        lanes = slice(i * leaf, (i + 1) * leaf)
        vec = vec_ref[:, lanes]
        first = first_ref[:, lanes]
        direction = grow * vec - step * first
        solution_ref[:, lanes] = step * vec + again * direction
        residual_ref[:, lanes] = (vec - step * first) - again * (grow * first - step * image)


def final_kernel(
    part_ref, group_ref, kah_ref, kal_ref, ubh_ref, ubl_ref, vec_ref, first_ref,
    solution_ref, residual_ref,
):
    second, share = second_image(part_ref, group_ref, kah_ref, kal_ref, ubh_ref, ubl_ref)
    update(group_ref, share, vec_ref, first_ref, second, solution_ref, residual_ref)


def last_kernel(part_ref, group_ref, kah_ref, kal_ref, ubh_ref, ubl_ref, second_ref, share_ref):
    second, share = second_image(part_ref, group_ref, kah_ref, kal_ref, ubh_ref, ubl_ref)
    second_ref[...] = jnp.concatenate(second, axis=1)
    share_ref[...] = jnp.broadcast_to(share, share_ref.shape)


def update_kernel(
    group_ref, share_ref, vec_ref, first_ref, second_ref, solution_ref, residual_ref
):
    update(
        group_ref, share_ref[:, 0:1], vec_ref, first_ref, [second_ref[...]],
        solution_ref, residual_ref,
    )


def vmem(count):
    return [pl.BlockSpec(memory_space=pltpu.VMEM)] * count


def smem(count):
    return [pl.BlockSpec(memory_space=pltpu.SMEM)] * count


def shape(*dims, dtype=F32):
    return jax.ShapeDtypeStruct(dims, dtype)


def pair(*dims):
    return [shape(*dims, dtype=BF16)] * 2


def call(kernel, outs, args, scalars=0, scratch=(), flops=0):
    return pl.pallas_call(
        kernel,
        out_shape=tuple(outs),
        in_specs=smem(scalars) + vmem(len(args) - scalars),
        out_specs=tuple(vmem(len(outs))),
        scratch_shapes=[pltpu.VMEM(dims, F32) for dims in scratch],
        compiler_params=pltpu.CompilerParams(vmem_limit_bytes=GRANT),
        cost_estimate=pl.CostEstimate(
            flops=flops, transcendentals=0, bytes_accessed=1000000
        ),
    )(*args)


def swap(x, axis, m):
    return lax.ppermute(x, axis, [(i, i ^ m) for i in range(lax.axis_size(axis))])


def sides(m4):
    nodes = lax.axis_size("sub") * lax.axis_size("leaf")
    across = [(q, q + 1) for q in range(1, nodes - 1, 2)]
    across = across + [(target, source) for source, target in across]
    return lax.ppermute(m4, ("leaf", "sub"), across)


def spread_groups(held):
    held = held[None]
    for offsets in exchange_rounds(lax.axis_size("leaf")):
        held = jnp.concatenate([held] + [swap(held, "leaf", offset) for offset in offsets], axis=0)
    return held


def far_memory(*args):
    return [pltpu.with_memory_space_constraint(x, pltpu.HBM) for x in args]


def shards(
    probe_rhs,
    coords,
    near_list,
    far_leaf_list,
    far_group_list,
    leaf_basis,
    leaf_skeleton,
    leaf_transfer,
    device_transfer,
    group_skeleton,
):
    leaves, rank, leaf = leaf_basis.shape
    probes, count = probe_rhs.shape
    groups = lax.axis_size("leaf")
    subs = lax.axis_size("sub")
    half = REACH * leaf
    span = leaves * rank
    base = span + LANE
    inside, across = window_tiles(leaves)
    transfer = leaf_transfer.reshape(span, rank)
    device = device_transfer[0]

    m1, own, m4, rhs, points, basis, transfer, device, near, far = call(
        first_kernel,
        [
            shape(probes + EXTRA, base + half),
            shape(probes + EXTRA, base),
            shape(probes + EXTRA, half),
            shape(probes, count),
            shape(EXTRA, count),
            shape(leaves, rank, leaf),
            shape(span, rank),
            shape(rank, rank),
            shape(*near_list.shape, dtype=jnp.int32),
            shape(*far_leaf_list.shape, dtype=jnp.int32),
        ],
        far_memory(
            far_group_list, probe_rhs, coords, leaf_skeleton, group_skeleton, leaf_basis,
            transfer, device, near_list, far_leaf_list,
        ),
        scalars=1,
    )
    r1, r2, r3 = swap(m1, "sub", 1), swap(own, "sub", 2), swap(own, "sub", 3)
    r4 = sides(m4)
    ubh, ubl = call(bases_kernel, pair(leaves, 2 * rank, leaf), (basis, transfer, device))
    th, tl = call(
        prepare_kernel, pair(len(inside) * leaf, leaf), (near, points), scratch=[(3, count, LANE)]
    )
    (term,) = call(term_kernel, [shape(probes // 2 + EXTRA, LANE)], (own, r1, r2, r3))
    gathered = spread_groups(term)
    klh, kll = call(
        skeleton_kernel,
        pair(subs * span, span),
        (far, own, r1, r2, r3),
        scratch=[(subs, 3, span, LANE)],
    )
    hh, hl = call(
        border_kernel,
        pair(len(across) * leaf, leaf),
        (near, r1, r4, points),
        scratch=[(EXTRA, 2 * half), (3, 2 * half, LANE)],
    )
    (inner,) = call(inner_kernel, [shape(probes, count)], (rhs, th, tl))
    (part,) = call(
        outer_kernel,
        [shape(probes, count)],
        (inner, own, r1, r2, r3, r4, hh, hl, klh, kll, ubh, ubl),
    )
    image, kgh, kgl, m4 = call(
        middle_kernel,
        [shape(probes, count)] + pair(rank, groups * rank) + [shape(probes, half)],
        (part, gathered, ubh, ubl),
        scratch=[(EXTRA, groups * rank), (3, LANE, LANE)],
    )
    r4 = sides(m4)
    m1, own = call(
        second_kernel, [shape(probes, base + half), shape(probes, base)], (image, ubh, ubl)
    )
    r1, r2, r3 = swap(m1, "sub", 1), swap(own, "sub", 2), swap(own, "sub", 3)
    dense = groups * rank <= DENSE
    if dense:
        kgh, kgl = call(
            groups_kernel,
            pair(groups * rank, groups * rank),
            (gathered,),
            scratch=[(EXTRA, groups * rank), (3, groups * rank, LANE)],
        )
    (inner,) = call(inner_kernel, [shape(probes, count)], (image, th, tl))
    part, message = call(
        local_kernel,
        [
            shape(probes, count),
            shape(groups * subs, probes // 2 // subs + SHARES, LANE),
        ],
        (rhs, image, inner, own, r1, r2, r3, r4, hh, hl, klh, kll, ubh, ubl),
    )
    gathered = lax.all_to_all(message, ("leaf", "sub"), 0, 0)
    outs = [shape(probes, count), shape(probes, count)]
    if dense:
        return call(final_kernel, outs, (part, gathered, kgh, kgl, ubh, ubl, rhs, image))
    second, share = call(
        last_kernel,
        [shape(probes, count), shape(probes, LANE)],
        (part, gathered, kgh, kgl, ubh, ubl),
    )
    share = lax.psum(share, "leaf")
    return call(update_kernel, outs, (gathered, share, rhs, image, second))


def solution(mesh):
    return jax.shard_map(
        shards,
        mesh=mesh,
        in_specs=(
            P(None, ("leaf", "sub")),
            P(None, ("leaf", "sub")),
            P(("leaf", "sub"), None),
            P(("leaf", "sub"), None),
            P("leaf", None),
            P(("leaf", "sub"), None, None),
            P(None, ("leaf", "sub")),
            P(("leaf", "sub"), None, None),
            P(("leaf", "sub"), None, None),
            P(None, "leaf"),
        ),
        out_specs=(P(None, ("leaf", "sub")), P(None, ("leaf", "sub"))),
        check_vma=False,
    )
```

```python
import jax
import jax.numpy as jnp
from jax import lax
from jax.experimental import pallas as pl
from jax.experimental.pallas import tpu as pltpu
from jax.sharding import PartitionSpec as P

REACH = 2
NOISE = 1.0
ROOT_FIVE = 5.0**0.5
LOG2_E = 1.4426950408889634
HIGHEST = lax.Precision.HIGHEST
F32 = jnp.float32
BF16 = jnp.bfloat16
DOWN = 2.0**-40
UP = 2.0**20
LANE = 128
EXTRA = 8
CHUNK = 32
UNROLL = 1024
SHARES = 4
GRANT = 16 * 2**20
DENSE = 1024


def dot(a, b, ca=1, cb=0):
    return lax.dot_general(
        a, b, (((ca,), (cb,)), ((), ())), precision=HIGHEST, preferred_element_type=F32
    )


def split(x):
    high = x.astype(BF16)
    return high, (x - high.astype(F32)).astype(BF16)


def stacked(x):
    return jnp.concatenate(split(x), axis=0)


def product(stack, high, low, transposed=False):
    rows = stack.shape[0] // 2
    dims = (((1,), (1 if transposed else 0,)), ((), ()))
    both = lax.dot_general(stack, high, dims, preferred_element_type=F32)
    more = lax.dot_general(stack[:rows], low, dims, preferred_element_type=F32)
    return (both[:rows] + both[rows:]) + more


def matern(rows, cols, weight):
    total = None
    for row, col in zip(rows, cols):
        spread = row - col
        total = spread * spread if total is None else total + spread * spread
    distance = total * lax.rsqrt(jnp.maximum(total, 1e-35))
    poly = (weight + (ROOT_FIVE * weight) * distance) + ((5.0 / 3.0) * weight) * total
    return poly * jnp.exp2((-ROOT_FIVE * LOG2_E) * distance)


def slot_columns(list_ref):
    leaves, slots = list_ref.shape
    block = jnp.full((EXTRA, LANE), -2, jnp.int32)
    tall = jnp.concatenate([list_ref[...], block[leaves:, 0:slots]], axis=0)
    wide = jnp.concatenate([tall, block[:, 0 : LANE - slots]], axis=1)
    return wide.T[0 : -(-slots // EXTRA) * EXTRA]


def named(columns, index):
    return jnp.max(jnp.where(columns == index, 1.0, 0.0).astype(F32), axis=0, keepdims=True)


def padded_lanes(x, lanes):
    return jnp.concatenate(
        [x, jnp.zeros((x.shape[0], lanes - x.shape[1]), x.dtype)], axis=1
    )


def padded_rows(x, rows):
    return jnp.concatenate(
        [x, jnp.zeros((rows - x.shape[0], x.shape[1]), x.dtype)], axis=0
    )


def ends(vec, half):
    even = lax.axis_index("sub") % 2 == 0
    low = vec[:, :half]
    high = vec[:, vec.shape[1] - half :]
    return jnp.where(even, high, low), jnp.where(even, low, high)


def write_row(ref, rows, *pieces):
    at = 0
    for piece in pieces:
        ref[rows, at : at + piece.shape[1]] = piece
        at = at + piece.shape[1]


def halos(r1, from_b, rows, base):
    odd = lax.axis_index("sub") % 2 == 1
    from_a = r1[rows, base:]
    return jnp.where(odd, from_a, from_b), jnp.where(odd, from_b, from_a)


def first_kernel(
    list_ref, vec_ref, coords_ref, skel_ref, gskel_ref, basis_ref, transfer_ref, device_ref,
    near_ref, far_ref,
    m1_ref, own_ref, m4_ref, rhs_ref, points_ref, basis_out, transfer_out, device_out,
    near_out, far_out, group_out,
):
    leaves, _, leaf = basis_ref.shape
    probes = vec_ref.shape[0]
    half = REACH * leaf
    vec = vec_ref[...]
    coefs = jnp.concatenate(
        [dot(vec[:, i * leaf : (i + 1) * leaf], basis_ref[i], 1, 1) for i in range(leaves)],
        axis=1,
    )
    term = fold_rows(dot(dot(coefs, transfer_ref[...]), device_ref[...]), leaves)
    relative = lax.axis_index("leaf") ^ lax.broadcasted_iota(jnp.int32, (1, LANE), 1)
    listed = jnp.zeros((1, LANE), F32)
    for column in range(list_ref.shape[1]):
        listed = jnp.where(relative == list_ref[0, column], 1.0, listed)
    group_rows = jnp.concatenate([padded_lanes(gskel_ref[...], LANE), listed], axis=0)
    points = padded_rows(coords_ref[...], EXTRA)
    skel = padded_rows(skel_ref[...], EXTRA)
    group_rows = padded_rows(group_rows, EXTRA)
    below = probes + term.shape[0]
    blank = jnp.zeros((EXTRA, 2 * half), F32)
    for rows, block, coordinates in (
        (slice(0, probes), coefs, vec),
        (slice(probes, below), term, points),
        (slice(below, below + EXTRA), skel, blank),
    ):
        part_a, part_b = ends(coordinates, half)
        write_row(m1_ref, rows, block, part_a)
        write_row(own_ref, rows, block)
        if rows.start < below:
            write_row(m4_ref, rows, part_b)
    group_out[...] = group_rows
    rhs_ref[...] = vec
    points_ref[...] = points
    basis_out[...] = basis_ref[...]
    transfer_out[...] = transfer_ref[...]
    device_out[...] = device_ref[...]
    near_out[...] = near_ref[...]
    far_out[...] = far_ref[...]


def spread_columns(points, wide_ref):
    columns = points.T
    for axis in range(3):
        wide_ref[axis] = jnp.broadcast_to(
            columns[:, axis : axis + 1], (columns.shape[0], LANE)
        )


def fill_tile(
    wide_ref, source, points_ref, top_row, lane, width, weight, pair, row, size, to=0
):
    high_ref, low_ref = pair

    def body(step, _):
        start = pl.multiple_of(source + step * CHUNK, CHUNK)
        target = pl.multiple_of(row + step * CHUNK, CHUNK)
        rows = [wide_ref[axis, pl.ds(start, CHUNK), :] for axis in range(3)]
        for at in range(0, width, LANE):
            cols = [
                points_ref[top_row + axis : top_row + axis + 1, lane + at : lane + at + LANE]
                for axis in range(3)
            ]
            factor = weight if weight.shape[1] == LANE else weight[:, at : at + LANE]
            top, rest = split(matern(rows, cols, factor))
            high_ref[pl.ds(target, CHUNK), to + at : to + at + LANE] = top
            low_ref[pl.ds(target, CHUNK), to + at : to + at + LANE] = rest
        return 0

    lax.fori_loop(0, size // CHUNK, body, 0, unroll=min(size // CHUNK, UNROLL // width))


def window_tiles(leaves):
    inside = []
    across = []
    for i in range(leaves):
        for j in range(i - REACH, i + REACH + 1):
            if not 0 <= j < leaves:
                across.append((i, j))
            elif j >= i:
                inside.append((i, j))
    return inside, across


def prepare_kernel(
    near_ref, points_ref, th_ref, tl_ref, wide_ref,
):
    leaves = near_ref.shape[0]
    leaf = points_ref.shape[1] // leaves
    first = (lax.axis_index("leaf") * lax.axis_size("sub") + lax.axis_index("sub")) * leaves
    spread_columns(points_ref[...], wide_ref)
    slots = slot_columns(near_ref)
    for at, (i, j) in enumerate(window_tiles(leaves)[0]):
        listed = jnp.broadcast_to(slots[:, i : i + 1], (slots.shape[0], LANE))
        fill_tile(
            wide_ref, j * leaf, points_ref, 0, i * leaf, leaf, named(listed, first + j),
            (th_ref, tl_ref), at * leaf, leaf,
        )


def bases_kernel(basis_ref, transfer_ref, device_ref, ubh_ref, ubl_ref):
    leaves, rank, _ = basis_ref.shape
    chain = dot(transfer_ref[...], device_ref[...])
    for i in range(leaves):
        basis = basis_ref[i]
        group_basis = dot(chain[i * rank : (i + 1) * rank], basis, 0, 0)
        top, rest = split(jnp.concatenate([basis, group_basis], axis=0))
        ubh_ref[i] = top
        ubl_ref[i] = rest


def fold_rows(x, parts):
    rows = x.shape[0] // parts
    return jnp.concatenate([x[r * rows : (r + 1) * rows] for r in range(parts)], axis=1)


def summed_terms(messages, probes, span):
    own, r1, r2, r3 = (ref[probes : probes + EXTRA, 0:span] for ref in messages)
    total = (own + r1) + (r2 + r3)
    return jnp.concatenate([total[:, at : at + LANE] for at in range(0, span, LANE)], axis=0)


def term_kernel(own, r1, r2, r3, group_rows, out_ref):
    half = out_ref.shape[0] - EXTRA
    probes = own.shape[0] - 2 * EXTRA
    out_ref[half:, :] = group_rows[...]
    out_ref[0:half, :] = summed_terms((own, r1, r2, r3), probes, own.shape[1])


def leaf_slice(x, i, leaf):
    return x[:, i * leaf : (i + 1) * leaf]


def inner_kernel(vec_ref, th_ref, tl_ref, out_ref):
    vec = vec_ref[...]
    leaf = th_ref.shape[1]
    leaves = vec.shape[1] // leaf
    stack = stacked(vec)
    totals = [NOISE * leaf_slice(vec, i, leaf) for i in range(leaves)]
    for at, (i, j) in enumerate(window_tiles(leaves)[0]):
        rows = slice(at * leaf, (at + 1) * leaf)
        high, low = th_ref[rows, :], tl_ref[rows, :]
        totals[i] = totals[i] + product(leaf_slice(stack, j, leaf), high, low)
        if j > i:
            totals[j] = totals[j] + product(leaf_slice(stack, i, leaf), high, low, True)
    out_ref[...] = jnp.concatenate(totals, axis=1)


def local_part(inner_ref, low, high, blocks, tiles, bases, out_ref):
    hh_ref, hl_ref, klh_ref, kll_ref = tiles
    ubh_ref, ubl_ref = bases
    leaves, double, leaf = ubh_ref.shape
    rank = double // 2
    across = window_tiles(leaves)[1]
    low, high = stacked(low), stacked(high)

    def piece(j):
        return leaf_slice(low, j + REACH, leaf) if j < 0 else leaf_slice(high, j - leaves, leaf)

    far = product(stacked(jnp.concatenate(blocks, axis=1)), klh_ref[...], kll_ref[...])
    far_stack = stacked(far)
    near = []
    for i in range(leaves):
        total = inner_ref[:, i * leaf : (i + 1) * leaf]
        at = [n for n, pair in enumerate(across) if pair[0] == i]
        if at:
            where = slice(at[0] * leaf, (at[-1] + 1) * leaf)
            wide = jnp.concatenate([piece(across[n][1]) for n in at], axis=1)
            total = total + product(wide, hh_ref[where, :], hl_ref[where, :])
        near.append(total)
        out_ref[:, i * leaf : (i + 1) * leaf] = total + product(
            far_stack[:, i * rank : (i + 1) * rank], ubh_ref[i, 0:rank, :], ubl_ref[i, 0:rank, :]
        )
    return jnp.concatenate(near, axis=1), far


def skeleton_kernel(far_ref, own, r1, r2, r3, klh_ref, kll_ref, wide_ref):
    leaves = far_ref.shape[0]
    span = klh_ref.shape[1]
    rank = span // leaves
    top = own.shape[0] - EXTRA
    sub = lax.axis_index("sub")
    group_first = lax.axis_index("leaf") * lax.axis_size("sub") * leaves
    messages = (own, r1, r2, r3)
    slots = slot_columns(far_ref)
    listed = jnp.concatenate(
        [jnp.broadcast_to(slots[:, i : i + 1], (slots.shape[0], rank)) for i in range(leaves)],
        axis=1,
    )
    for m, message in enumerate(messages):
        spread_columns(message[top : top + EXTRA, 0:span], wide_ref.at[m])
    for m in range(len(messages)):
        for j in range(leaves):
            index = group_first + (sub ^ m) * leaves + j
            fill_tile(
                wide_ref.at[m], j * rank, own, top, 0, span, named(listed, index),
                (klh_ref, kll_ref), m * span + j * rank, rank,
            )


def border_kernel(near_ref, r1, r4, points_ref, hh_ref, hl_ref, ends_ref, wide_ref):
    leaves = near_ref.shape[0]
    count = points_ref.shape[1]
    leaf = count // leaves
    half = REACH * leaf
    probes = r4.shape[0] - EXTRA
    first = (lax.axis_index("leaf") * lax.axis_size("sub") + lax.axis_index("sub")) * leaves
    rows = slice(probes, probes + EXTRA)
    low, high = halos(r1, r4[rows, :], rows, r1.shape[1] - half)
    ends_ref[:, 0:half] = low
    ends_ref[:, half:] = high
    spread_columns(ends_ref[...], wide_ref)
    slots = slot_columns(near_ref)
    for at, (i, j) in enumerate(window_tiles(leaves)[1]):
        listed = jnp.broadcast_to(slots[:, i : i + 1], (slots.shape[0], LANE))
        source = (j + REACH) * leaf if j < 0 else half + (j - leaves) * leaf
        fill_tile(
            wide_ref, source, points_ref, 0, i * leaf, leaf, named(listed, first + j),
            (hh_ref, hl_ref), at * leaf, leaf,
        )


def outer_kernel(
    inner_ref, own, r1, r2, r3, r4, hh_ref, hl_ref, klh_ref, kll_ref, ubh_ref, ubl_ref,
    part_ref,
):
    span = klh_ref.shape[1]
    rows = slice(0, inner_ref.shape[0])
    low, high = halos(r1, r4[rows, :], rows, own.shape[1])
    local_part(
        inner_ref, low, high, [r[rows, 0:span] for r in (own, r1, r2, r3)],
        (hh_ref, hl_ref, klh_ref, kll_ref), (ubh_ref, ubl_ref), part_ref,
    )


def row_sum(x):
    return jnp.sum(x, axis=1, keepdims=True)


def local_kernel(
    rhs_ref, vec_ref, inner_ref, own, r1, r2, r3, r4, hh_ref, hl_ref, klh_ref, kll_ref,
    ubh_ref, ubl_ref, part_ref, message_ref,
):
    base = own.shape[1]
    span = klh_ref.shape[1]
    rows = slice(0, vec_ref.shape[0])
    rhs = rhs_ref[...]
    vec = vec_ref[...]
    low, high = halos(r1, r4[...], rows, base)
    blocks = [r[rows, 0:span] for r in (own, r1, r2, r3)]
    near, far = local_part(
        inner_ref, low, high, blocks,
        (hh_ref, hl_ref, klh_ref, kll_ref), (ubh_ref, ubl_ref), part_ref,
    )
    shares = (
        row_sum(rhs * rhs),
        row_sum(rhs * vec),
        row_sum(vec * vec),
        row_sum((DOWN * vec) * near) + row_sum((DOWN * blocks[0]) * far),
    )
    lane = lax.broadcasted_iota(jnp.int32, (vec.shape[0], LANE), 1)
    columns = jnp.zeros((vec.shape[0], LANE), F32)
    for at, share in enumerate(shares):
        columns = jnp.where(lane == at, share, columns)
    term = summed_terms((own, r1, r2, r3), vec.shape[0], span)
    size = term.shape[0] // lax.axis_size("sub")
    sub = lax.axis_index("sub")
    mine = term[0:size]
    for m in range(1, lax.axis_size("sub")):
        mine = jnp.where(sub == m, term[m * size : (m + 1) * size], mine)
    flat = columns.T
    pieces = [mine[r : r + 1] for r in range(size)]
    pieces = pieces + [flat[at : at + 1, 0 : vec.shape[0]] for at in range(SHARES)]
    message = jnp.concatenate(pieces, axis=1)
    for m in range(message_ref.shape[0]):
        message_ref[m] = message


def exchange_order(groups):
    order = [0]
    for offsets in exchange_rounds(groups):
        order = order + [m ^ offset for offset in offsets for m in order]
    return order


def exchange_rounds(groups):
    return [[groups >> n] for n in range(1, groups.bit_length())]


def group_points(group_ref, half, rank):
    groups = group_ref.shape[0]
    return jnp.concatenate(
        [group_ref[m, half : half + EXTRA, 0:rank] for m in range(groups)], axis=1
    )


def group_row(group_ref, half, rank, leaves):
    size = half * LANE // (leaves * rank)
    return jnp.concatenate(
        [
            jnp.concatenate(
                [group_ref[m, row : row + size, at : at + rank] for m in range(group_ref.shape[0])],
                axis=1,
            )
            for row in range(0, half, size)
            for at in range(0, LANE, rank)
        ],
        axis=0,
    )


def group_mask(group_ref, row, block, rank):
    groups = group_ref.shape[0]
    order = exchange_order(groups)
    listed = group_ref[block, row : row + 1, :]
    lane_group = lax.broadcasted_iota(jnp.int32, (1, groups * rank), 1) // rank
    mask = jnp.zeros((1, groups * rank), F32)
    for m in range(block + 1, groups):
        at = order[block] ^ order[m]
        mask = jnp.where(lane_group == m, listed[:, at : at + 1], mask)
    return mask


def middle_kernel(
    part_ref, group_ref, ubh_ref, ubl_ref, image_ref, kgh_ref, kgl_ref, m4_ref,
    points_ref, wide_ref,
):
    leaves, double, leaf = ubh_ref.shape
    rank = double // 2
    groups = group_ref.shape[0]
    half = part_ref.shape[0] // 2
    points_ref[...] = group_points(group_ref, half, rank)
    spread_columns(group_ref[0, half : half + EXTRA, :], wide_ref)
    fill_tile(
        wide_ref, 0, points_ref, 0, 0, groups * rank,
        group_mask(group_ref, half + 3, 0, rank), (kgh_ref, kgl_ref), 0, rank,
    )
    held = group_row(group_ref, half, rank, leaves)
    group_far = product(stacked(held), kgh_ref[...], kgl_ref[...], True)
    group_stack = stacked(group_far)
    image = jnp.concatenate(
        [
            part_ref[:, i * leaf : (i + 1) * leaf]
            + product(group_stack, ubh_ref[i, rank:, :], ubl_ref[i, rank:, :])
            for i in range(leaves)
        ],
        axis=1,
    )
    image_ref[...] = image
    m4_ref[...] = ends(image, m4_ref.shape[1])[1]


def second_kernel(vec_ref, ubh_ref, ubl_ref, m1_ref, own_ref):
    leaves, double, leaf = ubh_ref.shape
    rank = double // 2
    vec = vec_ref[...]
    coefs = []
    term = None
    for i in range(leaves):
        both = product(stacked(leaf_slice(vec, i, leaf)), ubh_ref[i], ubl_ref[i], True)
        coefs.append(both[:, :rank])
        term = both if term is None else term + both
    coefs = jnp.concatenate(coefs, axis=1)
    term = fold_rows(term[:, rank:], leaves)
    probes = vec.shape[0]
    write_row(own_ref, slice(0, probes), coefs)
    write_row(own_ref, slice(probes, probes + EXTRA), term)
    write_row(m1_ref, slice(0, probes), coefs, ends(vec, REACH * leaf)[0])
    blank = jnp.zeros((EXTRA, REACH * leaf), F32)
    write_row(m1_ref, slice(probes, probes + EXTRA), term, blank)


def groups_kernel(group_ref, kah_ref, kal_ref, points_ref, wide_ref):
    groups, rows, _ = group_ref.shape
    rank = kah_ref.shape[0] // groups
    half = rows - EXTRA
    points_ref[...] = group_points(group_ref, half, rank)
    spread_columns(points_ref[...], wide_ref)
    kah_ref[...] = jnp.zeros(kah_ref.shape, BF16)
    kal_ref[...] = jnp.zeros(kal_ref.shape, BF16)
    for m in range(groups - 1):
        lane = (m + 1) * rank // LANE * LANE
        mask = group_mask(group_ref, half + 3, m, rank)
        fill_tile(
            wide_ref, m * rank, points_ref, 0, lane, groups * rank - lane, mask[:, lane:],
            (kah_ref, kal_ref), m * rank, rank, lane,
        )


def second_image(part_ref, group_ref, kgh_ref, kgl_ref, ubh_ref, ubl_ref, rows_ref, pairs):
    leaves, double, leaf = ubh_ref.shape
    rank = double // 2
    subs = lax.axis_size("sub")
    groups, half, _ = rows_ref.shape
    size = half // subs
    mine = lax.axis_index("leaf")
    for place, m in enumerate(exchange_order(groups)):
        for row in range(half):
            lane = row % size * LANE
            rows_ref[place, row : row + 1, :] = group_ref[
                (mine ^ m) * subs + row // size, :, lane : lane + LANE
            ]
    held = group_row(rows_ref, half, rank, leaves)
    stack = stacked(held)
    far = product(stack, kgh_ref[...], kgl_ref[...], True)
    group_stack = stacked(far)
    second = [
        part_ref[:, i * leaf : (i + 1) * leaf]
        + product(group_stack, ubh_ref[i, rank:, :], ubl_ref[i, rank:, :])
        for i in range(leaves)
    ]
    if not pairs:
        return second, row_sum((DOWN * held[:, :rank]) * far)
    ahead = product(stack, *(ref[...] for ref in pairs))
    return second, row_sum((2.0 * DOWN * held) * ahead)


def update(group_ref, share, vec_ref, first_ref, second, solution_ref, residual_ref):
    probes = vec_ref.shape[0]
    start = group_ref.shape[2] - SHARES * probes
    total = group_ref[0, :, start:]
    for q in range(1, group_ref.shape[0]):
        total = total + group_ref[q, :, start:]
    pieces = [total[:, at : at + probes] for at in range(0, SHARES * probes, probes)]
    sums = padded_lanes(padded_rows(jnp.concatenate(pieces, axis=0), EXTRA), LANE).T
    bb, bw, ww, wv = (sums[0:probes, k : k + 1] for k in range(SHARES))
    wv = wv + share
    step = bb / bw
    rise = (step * ww) * step
    norm = rise - bb
    grow = rise / bb
    scaled = step * UP
    curvature = (grow * grow) * bw - (2.0 * grow) * (step * ww) + (scaled * wv) * scaled
    again = norm / curvature
    leaf = second[0].shape[1]
    for i, image in enumerate(second):
        lanes = slice(i * leaf, (i + 1) * leaf)
        vec = vec_ref[:, lanes]
        first = first_ref[:, lanes]
        direction = grow * vec - step * first
        solution_ref[:, lanes] = step * vec + again * direction
        residual_ref[:, lanes] = (vec - step * first) - again * (grow * first - step * image)


def final_kernel(
    part_ref, group_ref, kgh_ref, kgl_ref, kah_ref, kal_ref, ubh_ref, ubl_ref, vec_ref,
    first_ref, solution_ref, residual_ref, rows_ref,
):
    second, share = second_image(
        part_ref, group_ref, kgh_ref, kgl_ref, ubh_ref, ubl_ref, rows_ref, (kah_ref, kal_ref)
    )
    update(group_ref, share, vec_ref, first_ref, second, solution_ref, residual_ref)


def last_kernel(
    part_ref, group_ref, kgh_ref, kgl_ref, ubh_ref, ubl_ref, second_ref, share_ref, rows_ref
):
    second, share = second_image(
        part_ref, group_ref, kgh_ref, kgl_ref, ubh_ref, ubl_ref, rows_ref, None
    )
    second_ref[...] = jnp.concatenate(second, axis=1)
    share_ref[...] = jnp.broadcast_to(share, share_ref.shape)


def update_kernel(
    group_ref, share_ref, vec_ref, first_ref, second_ref, solution_ref, residual_ref
):
    update(
        group_ref, share_ref[:, 0:1], vec_ref, first_ref, [second_ref[...]],
        solution_ref, residual_ref,
    )


def vmem(count):
    return [pl.BlockSpec(memory_space=pltpu.VMEM)] * count


def smem(count):
    return [pl.BlockSpec(memory_space=pltpu.SMEM)] * count


def shape(*dims, dtype=F32):
    return jax.ShapeDtypeStruct(dims, dtype)


def pair(*dims):
    return [shape(*dims, dtype=BF16)] * 2


def call(kernel, outs, args, scalars=0, scratch=(), flops=0):
    return pl.pallas_call(
        kernel,
        out_shape=tuple(outs),
        in_specs=smem(scalars) + vmem(len(args) - scalars),
        out_specs=tuple(vmem(len(outs))),
        scratch_shapes=[pltpu.VMEM(dims, F32) for dims in scratch],
        compiler_params=pltpu.CompilerParams(vmem_limit_bytes=GRANT),
        cost_estimate=pl.CostEstimate(
            flops=flops, transcendentals=0, bytes_accessed=1000000
        ),
    )(*args)


def swap(x, axis, m):
    return lax.ppermute(x, axis, [(i, i ^ m) for i in range(lax.axis_size(axis))])


def sides(m4):
    nodes = lax.axis_size("sub") * lax.axis_size("leaf")
    across = [(q, q + 1) for q in range(1, nodes - 1, 2)]
    across = across + [(target, source) for source, target in across]
    return lax.ppermute(m4, ("leaf", "sub"), across)


def spread_groups(held):
    held = held[None]
    for offsets in exchange_rounds(lax.axis_size("leaf")):
        held = jnp.concatenate([held] + [swap(held, "leaf", offset) for offset in offsets], axis=0)
    return held


def far_memory(*args):
    return [pltpu.with_memory_space_constraint(x, pltpu.HBM) for x in args]


def shards(
    probe_rhs,
    coords,
    near_list,
    far_leaf_list,
    far_group_list,
    leaf_basis,
    leaf_skeleton,
    leaf_transfer,
    device_transfer,
    group_skeleton,
):
    leaves, rank, leaf = leaf_basis.shape
    probes, count = probe_rhs.shape
    groups = lax.axis_size("leaf")
    subs = lax.axis_size("sub")
    half = REACH * leaf
    span = leaves * rank
    inside, across = window_tiles(leaves)
    transfer = leaf_transfer.reshape(span, rank)
    device = device_transfer[0]

    m1, own, m4, rhs, points, basis, transfer, device, near, far, group_rows = call(
        first_kernel,
        [
            shape(probes + 2 * EXTRA, span + half),
            shape(probes + 2 * EXTRA, span),
            shape(probes + EXTRA, half),
            shape(probes, count),
            shape(EXTRA, count),
            shape(leaves, rank, leaf),
            shape(span, rank),
            shape(rank, rank),
            shape(*near_list.shape, dtype=jnp.int32),
            shape(*far_leaf_list.shape, dtype=jnp.int32),
            shape(EXTRA, LANE),
        ],
        far_memory(
            far_group_list, probe_rhs, coords, leaf_skeleton, group_skeleton, leaf_basis,
            transfer, device, near_list, far_leaf_list,
        ),
        scalars=1,
    )
    r1, r2, r3 = swap(m1, "sub", 1), swap(own, "sub", 2), swap(own, "sub", 3)
    r4 = sides(m4)
    ubh, ubl = call(bases_kernel, pair(leaves, 2 * rank, leaf), (basis, transfer, device))
    th, tl = call(
        prepare_kernel, pair(len(inside) * leaf, leaf), (near, points), scratch=[(3, count, LANE)]
    )
    (term,) = call(term_kernel, [shape(probes // 2 + EXTRA, LANE)], (own, r1, r2, r3, group_rows))
    gathered = spread_groups(term)
    klh, kll = call(
        skeleton_kernel,
        pair(subs * span, span),
        (far, own, r1, r2, r3),
        scratch=[(subs, 3, span, LANE)],
    )
    hh, hl = call(
        border_kernel,
        pair(len(across) * leaf, leaf),
        (near, r1, r4, points),
        scratch=[(EXTRA, 2 * half), (3, 2 * half, LANE)],
    )
    (inner,) = call(inner_kernel, [shape(probes, count)], (rhs, th, tl))
    (part,) = call(
        outer_kernel,
        [shape(probes, count)],
        (inner, own, r1, r2, r3, r4, hh, hl, klh, kll, ubh, ubl),
    )
    image, kgh, kgl, m4 = call(
        middle_kernel,
        [shape(probes, count)] + pair(rank, groups * rank) + [shape(probes, half)],
        (part, gathered, ubh, ubl),
        scratch=[(EXTRA, groups * rank), (3, LANE, LANE)],
    )
    r4 = sides(m4)
    m1, own = call(
        second_kernel,
        [shape(probes + EXTRA, span + half), shape(probes + EXTRA, span)],
        (image, ubh, ubl),
    )
    r1, r2, r3 = swap(m1, "sub", 1), swap(own, "sub", 2), swap(own, "sub", 3)
    dense = groups * rank <= DENSE
    if dense:
        kah, kal = call(
            groups_kernel,
            pair(groups * rank, groups * rank),
            (gathered,),
            scratch=[(EXTRA, groups * rank), (3, groups * rank, LANE)],
        )
    (inner,) = call(inner_kernel, [shape(probes, count)], (image, th, tl))
    part, message = call(
        local_kernel,
        [
            shape(probes, count),
            shape(groups * subs, 1, probes // 2 // subs * LANE + SHARES * probes),
        ],
        (rhs, image, inner, own, r1, r2, r3, r4, hh, hl, klh, kll, ubh, ubl),
    )
    gathered = lax.all_to_all(message, ("leaf", "sub"), 0, 0)
    outs = [shape(probes, count), shape(probes, count)]
    if dense:
        return call(
            final_kernel,
            outs,
            (part, gathered, kgh, kgl, kah, kal, ubh, ubl, rhs, image),
            scratch=[(groups, probes // 2, LANE)],
        )
    second, share = call(
        last_kernel,
        [shape(probes, count), shape(probes, LANE)],
        (part, gathered, kgh, kgl, ubh, ubl),
        scratch=[(groups, probes // 2, LANE)],
    )
    share = lax.psum(share, "leaf")
    return call(update_kernel, outs, (gathered, share, rhs, image, second))


def solution(mesh):
    return jax.shard_map(
        shards,
        mesh=mesh,
        in_specs=(
            P(None, ("leaf", "sub")),
            P(None, ("leaf", "sub")),
            P(("leaf", "sub"), None),
            P(("leaf", "sub"), None),
            P("leaf", None),
            P(("leaf", "sub"), None, None),
            P(None, ("leaf", "sub")),
            P(("leaf", "sub"), None, None),
            P(("leaf", "sub"), None, None),
            P(None, "leaf"),
        ),
        out_specs=(P(None, ("leaf", "sub")), P(None, ("leaf", "sub"))),
        check_vma=False,
    )
```

```python
import jax
import jax.numpy as jnp
from jax import lax
from jax.experimental import pallas as pl
from jax.experimental.pallas import tpu as pltpu
from jax.sharding import PartitionSpec as P

REACH = 2
NOISE = 1.0
ROOT_FIVE = 5.0**0.5
LOG2_E = 1.4426950408889634
HIGHEST = lax.Precision.HIGHEST
F32 = jnp.float32
BF16 = jnp.bfloat16
DOWN = 2.0**-40
UP = 2.0**20
LANE = 128
EXTRA = 8
CHUNK = 32
UNROLL = 2048
SHARES = 4
GRANT = 16 * 2**20
DENSE = 1024


def dot(a, b, ca=1, cb=0):
    return lax.dot_general(
        a, b, (((ca,), (cb,)), ((), ())), precision=HIGHEST, preferred_element_type=F32
    )


def split(x):
    high = x.astype(BF16)
    return high, (x - high.astype(F32)).astype(BF16)


def stacked(x):
    return jnp.concatenate(split(x), axis=0)


def product(stack, high, low, transposed=False):
    rows = stack.shape[0] // 2
    dims = (((1,), (1 if transposed else 0,)), ((), ()))
    both = lax.dot_general(stack, high, dims, preferred_element_type=F32)
    more = lax.dot_general(stack[:rows], low, dims, preferred_element_type=F32)
    return (both[:rows] + both[rows:]) + more


def matern(rows, cols, weight):
    total = None
    for row, col in zip(rows, cols):
        spread = row - col
        total = spread * spread if total is None else total + spread * spread
    distance = total * lax.rsqrt(jnp.maximum(total, 1e-35))
    poly = (weight + (ROOT_FIVE * weight) * distance) + ((5.0 / 3.0) * weight) * total
    return poly * jnp.exp2((-ROOT_FIVE * LOG2_E) * distance)


def slot_columns(list_ref):
    leaves, slots = list_ref.shape
    block = jnp.full((EXTRA, LANE), -2, jnp.int32)
    tall = jnp.concatenate([list_ref[...], block[leaves:, 0:slots]], axis=0)
    wide = jnp.concatenate([tall, block[:, 0 : LANE - slots]], axis=1)
    return wide.T[0 : -(-slots // EXTRA) * EXTRA]


def named(columns, index):
    return jnp.max(jnp.where(columns == index, 1.0, 0.0).astype(F32), axis=0, keepdims=True)


def near_weights(near_ref, first, pairs):
    slots = slot_columns(near_ref)
    listed = [
        jnp.broadcast_to(slots[:, i : i + 1], (slots.shape[0], LANE))
        for i in range(near_ref.shape[0])
    ]
    return [named(listed[i], first + j) for i, j in pairs]


def padded_lanes(x, lanes):
    return jnp.concatenate(
        [x, jnp.zeros((x.shape[0], lanes - x.shape[1]), x.dtype)], axis=1
    )


def padded_rows(x, rows):
    return jnp.concatenate(
        [x, jnp.zeros((rows - x.shape[0], x.shape[1]), x.dtype)], axis=0
    )


def ends(vec, half):
    even = lax.axis_index("sub") % 2 == 0
    low = vec[:, :half]
    high = vec[:, vec.shape[1] - half :]
    return jnp.where(even, high, low), jnp.where(even, low, high)


def write_row(ref, rows, *pieces):
    at = 0
    for piece in pieces:
        ref[rows, at : at + piece.shape[1]] = piece
        at = at + piece.shape[1]


def halos(r1, from_b, rows, base):
    odd = lax.axis_index("sub") % 2 == 1
    from_a = r1[rows, base:]
    return jnp.where(odd, from_a, from_b), jnp.where(odd, from_b, from_a)


def first_kernel(
    list_ref, vec_ref, coords_ref, skel_ref, gskel_ref, basis_ref, transfer_ref, device_ref,
    near_ref, far_ref,
    m1_ref, own_ref, m4_ref, rhs_ref, points_ref, basis_out, transfer_out, device_out,
    near_out, far_out, group_out,
):
    leaves, _, leaf = basis_ref.shape
    probes = vec_ref.shape[0]
    half = REACH * leaf
    vec = vec_ref[...]
    coefs = jnp.concatenate(
        [
            product(stacked(vec[:, i * leaf : (i + 1) * leaf]), *split(basis_ref[i]), True)
            for i in range(leaves)
        ],
        axis=1,
    )
    term = fold_rows(dot(dot(coefs, transfer_ref[...]), device_ref[...]), leaves)
    relative = lax.axis_index("leaf") ^ lax.broadcasted_iota(jnp.int32, (1, LANE), 1)
    listed = jnp.zeros((1, LANE), F32)
    for column in range(list_ref.shape[1]):
        listed = jnp.where(relative == list_ref[0, column], 1.0, listed)
    group_rows = jnp.concatenate([padded_lanes(gskel_ref[...], LANE), listed], axis=0)
    points = padded_rows(coords_ref[...], EXTRA)
    skel = padded_rows(skel_ref[...], EXTRA)
    group_rows = padded_rows(group_rows, EXTRA)
    below = probes + term.shape[0]
    blank = jnp.zeros((EXTRA, 2 * half), F32)
    for rows, block, coordinates in (
        (slice(0, probes), coefs, vec),
        (slice(probes, below), term, points),
        (slice(below, below + EXTRA), skel, blank),
    ):
        part_a, part_b = ends(coordinates, half)
        write_row(m1_ref, rows, block, part_a)
        write_row(own_ref, rows, block)
        if rows.start < below:
            write_row(m4_ref, rows, part_b)
    group_out[...] = group_rows
    rhs_ref[...] = vec
    points_ref[...] = points
    basis_out[...] = basis_ref[...]
    transfer_out[...] = transfer_ref[...]
    device_out[...] = device_ref[...]
    near_out[...] = near_ref[...]
    far_out[...] = far_ref[...]


def spread_columns(points, wide_ref):
    columns = points.T
    for axis in range(3):
        wide_ref[axis] = jnp.broadcast_to(
            columns[:, axis : axis + 1], (columns.shape[0], LANE)
        )


def fill_tile(
    wide_ref, source, points_ref, top_row, lane, width, weight, pair, row, size, to=0
):
    high_ref, low_ref = pair

    def body(step, _):
        start = pl.multiple_of(source + step * CHUNK, CHUNK)
        target = pl.multiple_of(row + step * CHUNK, CHUNK)
        rows = [wide_ref[axis, pl.ds(start, CHUNK), :] for axis in range(3)]
        for at in range(0, width, LANE):
            cols = [
                points_ref[top_row + axis : top_row + axis + 1, lane + at : lane + at + LANE]
                for axis in range(3)
            ]
            factor = weight if weight.shape[1] == LANE else weight[:, at : at + LANE]
            top, rest = split(matern(rows, cols, factor))
            high_ref[pl.ds(target, CHUNK), to + at : to + at + LANE] = top
            low_ref[pl.ds(target, CHUNK), to + at : to + at + LANE] = rest
        return 0

    lax.fori_loop(0, size // CHUNK, body, 0, unroll=min(size // CHUNK, UNROLL // width))


def window_tiles(leaves):
    inside = []
    across = []
    for i in range(leaves):
        for j in range(i - REACH, i + REACH + 1):
            if not 0 <= j < leaves:
                across.append((i, j))
            elif j >= i:
                inside.append((i, j))
    return inside, across


def prepare_kernel(
    near_ref, points_ref, th_ref, tl_ref, wide_ref,
):
    leaves = near_ref.shape[0]
    leaf = points_ref.shape[1] // leaves
    first = (lax.axis_index("leaf") * lax.axis_size("sub") + lax.axis_index("sub")) * leaves
    spread_columns(points_ref[...], wide_ref)
    pairs = window_tiles(leaves)[0]
    weights = near_weights(near_ref, first, pairs)
    for at, (i, j) in enumerate(pairs):
        fill_tile(
            wide_ref, j * leaf, points_ref, 0, i * leaf, leaf, weights[at],
            (th_ref, tl_ref), at * leaf, leaf,
        )


def bases_kernel(basis_ref, transfer_ref, device_ref, ubh_ref, ubl_ref):
    leaves, rank, _ = basis_ref.shape
    chain = stacked(dot(device_ref[...], transfer_ref[...], 0, 1))
    for i in range(leaves):
        top, rest = split(basis_ref[i])
        group_basis = product(chain[:, i * rank : (i + 1) * rank], top, rest)
        group_top, group_rest = split(group_basis)
        ubh_ref[i] = jnp.concatenate([top, group_top], axis=0)
        ubl_ref[i] = jnp.concatenate([rest, group_rest], axis=0)


def fold_rows(x, parts):
    rows = x.shape[0] // parts
    return jnp.concatenate([x[r * rows : (r + 1) * rows] for r in range(parts)], axis=1)


def summed_terms(messages, probes, span):
    own, r1, r2, r3 = (ref[probes : probes + EXTRA, 0:span] for ref in messages)
    total = (own + r1) + (r2 + r3)
    return jnp.concatenate([total[:, at : at + LANE] for at in range(0, span, LANE)], axis=0)


def term_kernel(own, r1, r2, r3, group_rows, out_ref):
    half = out_ref.shape[0] - EXTRA
    probes = own.shape[0] - 2 * EXTRA
    out_ref[half:, :] = group_rows[...]
    out_ref[0:half, :] = summed_terms((own, r1, r2, r3), probes, own.shape[1])


def leaf_slice(x, i, leaf):
    return x[:, i * leaf : (i + 1) * leaf]


def columns_of(shares, rows):
    lane = lax.broadcasted_iota(jnp.int32, (rows, LANE), 1)
    columns = jnp.zeros((rows, LANE), F32)
    for at, share in enumerate(shares):
        columns = jnp.where(lane == at, share, columns)
    return columns


def again_kernel(rhs_ref, vec_ref, th_ref, tl_ref, out_ref, columns_ref):
    rhs = rhs_ref[...]
    vec = vec_ref[...]
    shares = row_sum(rhs * rhs), row_sum(rhs * vec), row_sum(vec * vec)
    columns_ref[...] = columns_of(shares, vec.shape[0])
    inner_kernel(vec_ref, th_ref, tl_ref, out_ref)


def inner_kernel(vec_ref, th_ref, tl_ref, out_ref):
    vec = vec_ref[...]
    leaf = th_ref.shape[1]
    leaves = vec.shape[1] // leaf
    stack = stacked(vec)
    totals = [NOISE * leaf_slice(vec, i, leaf) for i in range(leaves)]
    for at, (i, j) in enumerate(window_tiles(leaves)[0]):
        rows = slice(at * leaf, (at + 1) * leaf)
        high, low = th_ref[rows, :], tl_ref[rows, :]
        totals[i] = totals[i] + product(leaf_slice(stack, j, leaf), high, low)
        if j > i:
            totals[j] = totals[j] + product(leaf_slice(stack, i, leaf), high, low, True)
    out_ref[...] = jnp.concatenate(totals, axis=1)


def local_part(inner_ref, low, high, blocks, tiles, bases, out_ref):
    hh_ref, hl_ref, klh_ref, kll_ref = tiles
    ubh_ref, ubl_ref = bases
    leaves, double, leaf = ubh_ref.shape
    rank = double // 2
    across = window_tiles(leaves)[1]
    low, high = stacked(low), stacked(high)

    def piece(j):
        return leaf_slice(low, j + REACH, leaf) if j < 0 else leaf_slice(high, j - leaves, leaf)

    far = product(stacked(jnp.concatenate(blocks, axis=1)), klh_ref[...], kll_ref[...])
    far_stack = stacked(far)
    near = []
    for i in range(leaves):
        total = inner_ref[:, i * leaf : (i + 1) * leaf]
        at = [n for n, pair in enumerate(across) if pair[0] == i]
        if at:
            where = slice(at[0] * leaf, (at[-1] + 1) * leaf)
            wide = jnp.concatenate([piece(across[n][1]) for n in at], axis=1)
            total = total + product(wide, hh_ref[where, :], hl_ref[where, :])
        near.append(total)
        out_ref[:, i * leaf : (i + 1) * leaf] = total + product(
            far_stack[:, i * rank : (i + 1) * rank], ubh_ref[i, 0:rank, :], ubl_ref[i, 0:rank, :]
        )
    return jnp.concatenate(near, axis=1), far


def skeleton_kernel(far_ref, own, r1, r2, r3, klh_ref, kll_ref, wide_ref):
    leaves = far_ref.shape[0]
    span = klh_ref.shape[1]
    rank = span // leaves
    top = own.shape[0] - EXTRA
    sub = lax.axis_index("sub")
    group_first = lax.axis_index("leaf") * lax.axis_size("sub") * leaves
    messages = (own, r1, r2, r3)
    slots = slot_columns(far_ref)
    listed = jnp.concatenate(
        [jnp.broadcast_to(slots[:, i : i + 1], (slots.shape[0], rank)) for i in range(leaves)],
        axis=1,
    )
    for m, message in enumerate(messages):
        spread_columns(message[top : top + EXTRA, 0:span], wide_ref.at[m])
    places = [(m, j) for m in range(len(messages)) for j in range(leaves)]
    masks = [named(listed, group_first + (sub ^ m) * leaves + j) for m, j in places]
    for mask, (m, j) in zip(masks, places):
        fill_tile(
            wide_ref.at[m], j * rank, own, top, 0, span, mask,
            (klh_ref, kll_ref), m * span + j * rank, rank,
        )


def border_kernel(near_ref, r1, r4, points_ref, hh_ref, hl_ref, ends_ref, wide_ref):
    leaves = near_ref.shape[0]
    count = points_ref.shape[1]
    leaf = count // leaves
    half = REACH * leaf
    probes = r4.shape[0] - EXTRA
    first = (lax.axis_index("leaf") * lax.axis_size("sub") + lax.axis_index("sub")) * leaves
    rows = slice(probes, probes + EXTRA)
    low, high = halos(r1, r4[rows, :], rows, r1.shape[1] - half)
    ends_ref[:, 0:half] = low
    ends_ref[:, half:] = high
    spread_columns(ends_ref[...], wide_ref)
    pairs = window_tiles(leaves)[1]
    weights = near_weights(near_ref, first, pairs)
    for at, (i, j) in enumerate(pairs):
        source = (j + REACH) * leaf if j < 0 else half + (j - leaves) * leaf
        fill_tile(
            wide_ref, source, points_ref, 0, i * leaf, leaf, weights[at],
            (hh_ref, hl_ref), at * leaf, leaf,
        )


def outer_kernel(
    inner_ref, own, r1, r2, r3, r4, hh_ref, hl_ref, klh_ref, kll_ref, ubh_ref, ubl_ref,
    part_ref,
):
    span = klh_ref.shape[1]
    rows = slice(0, inner_ref.shape[0])
    low, high = halos(r1, r4[rows, :], rows, own.shape[1])
    local_part(
        inner_ref, low, high, [r[rows, 0:span] for r in (own, r1, r2, r3)],
        (hh_ref, hl_ref, klh_ref, kll_ref), (ubh_ref, ubl_ref), part_ref,
    )


def row_sum(x):
    return jnp.sum(x, axis=1, keepdims=True)


def local_kernel(
    columns_ref, vec_ref, inner_ref, own, r1, r2, r3, r4, hh_ref, hl_ref, klh_ref, kll_ref,
    ubh_ref, ubl_ref, part_ref, message_ref,
):
    base = own.shape[1]
    span = klh_ref.shape[1]
    rows = slice(0, vec_ref.shape[0])
    vec = vec_ref[...]
    low, high = halos(r1, r4[...], rows, base)
    blocks = [r[rows, 0:span] for r in (own, r1, r2, r3)]
    near, far = local_part(
        inner_ref, low, high, blocks,
        (hh_ref, hl_ref, klh_ref, kll_ref), (ubh_ref, ubl_ref), part_ref,
    )
    share = row_sum((DOWN * vec) * near) + row_sum((DOWN * blocks[0]) * far)
    lane = lax.broadcasted_iota(jnp.int32, columns_ref.shape, 1)
    columns = jnp.where(lane == SHARES - 1, share, columns_ref[...])
    term = summed_terms((own, r1, r2, r3), vec.shape[0], span)
    size = term.shape[0] // lax.axis_size("sub")
    sub = lax.axis_index("sub")
    mine = term[0:size]
    for m in range(1, lax.axis_size("sub")):
        mine = jnp.where(sub == m, term[m * size : (m + 1) * size], mine)
    flat = columns.T
    pieces = [mine[r : r + 1] for r in range(size)]
    pieces = pieces + [flat[at : at + 1, 0 : vec.shape[0]] for at in range(SHARES)]
    message = jnp.concatenate(pieces, axis=1)
    for m in range(message_ref.shape[0]):
        message_ref[m] = message


def exchange_order(groups):
    order = [0]
    for offsets in exchange_rounds(groups):
        order = order + [m ^ offset for offset in offsets for m in order]
    return order


def exchange_rounds(groups):
    if groups == 8:
        return [[2, 4, 6], [1]]
    return [[groups >> n] for n in range(1, groups.bit_length())]


def group_points(group_ref, half, rank):
    groups = group_ref.shape[0]
    return jnp.concatenate(
        [group_ref[m, half : half + EXTRA, 0:rank] for m in range(groups)], axis=1
    )


def group_row(group_ref, half, rank, leaves):
    size = half * LANE // (leaves * rank)
    return jnp.concatenate(
        [
            jnp.concatenate(
                [group_ref[m, row : row + size, at : at + rank] for m in range(group_ref.shape[0])],
                axis=1,
            )
            for row in range(0, half, size)
            for at in range(0, LANE, rank)
        ],
        axis=0,
    )


def group_mask(group_ref, row, block, rank):
    groups = group_ref.shape[0]
    order = exchange_order(groups)
    listed = group_ref[block, row : row + 1, :]
    lane_group = lax.broadcasted_iota(jnp.int32, (1, groups * rank), 1) // rank
    mask = jnp.zeros((1, groups * rank), F32)
    for m in range(block + 1, groups):
        at = order[block] ^ order[m]
        mask = jnp.where(lane_group == m, listed[:, at : at + 1], mask)
    return mask


def middle_kernel(
    part_ref, group_ref, ubh_ref, ubl_ref, image_ref, kgh_ref, kgl_ref, m4_ref,
    points_ref, wide_ref,
):
    leaves, double, leaf = ubh_ref.shape
    rank = double // 2
    groups = group_ref.shape[0]
    half = part_ref.shape[0] // 2
    points_ref[...] = group_points(group_ref, half, rank)
    spread_columns(group_ref[0, half : half + EXTRA, :], wide_ref)
    fill_tile(
        wide_ref, 0, points_ref, 0, 0, groups * rank,
        group_mask(group_ref, half + 3, 0, rank), (kgh_ref, kgl_ref), 0, rank,
    )
    held = group_row(group_ref, half, rank, leaves)
    group_far = product(stacked(held), kgh_ref[...], kgl_ref[...], True)
    group_stack = stacked(group_far)
    image = jnp.concatenate(
        [
            part_ref[:, i * leaf : (i + 1) * leaf]
            + product(group_stack, ubh_ref[i, rank:, :], ubl_ref[i, rank:, :])
            for i in range(leaves)
        ],
        axis=1,
    )
    image_ref[...] = image
    m4_ref[...] = ends(image, m4_ref.shape[1])[1]


def second_kernel(vec_ref, ubh_ref, ubl_ref, m1_ref, own_ref):
    leaves, double, leaf = ubh_ref.shape
    rank = double // 2
    vec = vec_ref[...]
    coefs = []
    term = None
    for i in range(leaves):
        both = product(stacked(leaf_slice(vec, i, leaf)), ubh_ref[i], ubl_ref[i], True)
        coefs.append(both[:, :rank])
        term = both if term is None else term + both
    coefs = jnp.concatenate(coefs, axis=1)
    term = fold_rows(term[:, rank:], leaves)
    probes = vec.shape[0]
    write_row(own_ref, slice(0, probes), coefs)
    write_row(own_ref, slice(probes, probes + EXTRA), term)
    write_row(m1_ref, slice(0, probes), coefs, ends(vec, REACH * leaf)[0])
    blank = jnp.zeros((EXTRA, REACH * leaf), F32)
    write_row(m1_ref, slice(probes, probes + EXTRA), term, blank)


def groups_kernel(group_ref, kah_ref, kal_ref, points_ref, wide_ref):
    groups, rows, _ = group_ref.shape
    rank = kah_ref.shape[0] // groups
    half = rows - EXTRA
    points_ref[...] = group_points(group_ref, half, rank)
    spread_columns(points_ref[...], wide_ref)
    kah_ref[...] = jnp.zeros(kah_ref.shape, BF16)
    kal_ref[...] = jnp.zeros(kal_ref.shape, BF16)
    masks = [group_mask(group_ref, half + 3, m, rank) for m in range(groups - 1)]
    for m, mask in enumerate(masks):
        lane = (m + 1) * rank // LANE * LANE
        fill_tile(
            wide_ref, m * rank, points_ref, 0, lane, groups * rank - lane, mask[:, lane:],
            (kah_ref, kal_ref), m * rank, rank, lane,
        )


def second_image(part_ref, group_ref, kgh_ref, kgl_ref, ubh_ref, ubl_ref, rows_ref, pairs):
    leaves, double, leaf = ubh_ref.shape
    rank = double // 2
    subs = lax.axis_size("sub")
    groups, half, _ = rows_ref.shape
    size = half // subs
    mine = lax.axis_index("leaf")
    for place, m in enumerate(exchange_order(groups)):
        for row in range(half):
            lane = row % size * LANE
            rows_ref[place, row : row + 1, :] = group_ref[
                (mine ^ m) * subs + row // size, :, lane : lane + LANE
            ]
    held = group_row(rows_ref, half, rank, leaves)
    stack = stacked(held)
    far = product(stack, kgh_ref[...], kgl_ref[...], True)
    group_stack = stacked(far)
    second = [
        part_ref[:, i * leaf : (i + 1) * leaf]
        + product(group_stack, ubh_ref[i, rank:, :], ubl_ref[i, rank:, :])
        for i in range(leaves)
    ]
    if not pairs:
        return second, row_sum((DOWN * held[:, :rank]) * far)
    ahead = product(stack, *(ref[...] for ref in pairs))
    return second, row_sum((2.0 * DOWN * held) * ahead)


def update(group_ref, share, vec_ref, first_ref, second, solution_ref, residual_ref):
    probes = vec_ref.shape[0]
    start = group_ref.shape[2] - SHARES * probes
    total = group_ref[0, :, start:]
    for q in range(1, group_ref.shape[0]):
        total = total + group_ref[q, :, start:]
    pieces = [total[:, at : at + probes] for at in range(0, SHARES * probes, probes)]
    sums = padded_lanes(padded_rows(jnp.concatenate(pieces, axis=0), EXTRA), LANE).T
    bb, bw, ww, wv = (sums[0:probes, k : k + 1] for k in range(SHARES))
    wv = wv + share
    step = bb / bw
    rise = (step * ww) * step
    norm = rise - bb
    grow = rise / bb
    scaled = step * UP
    curvature = (grow * grow) * bw - (2.0 * grow) * (step * ww) + (scaled * wv) * scaled
    again = norm / curvature
    leaf = second[0].shape[1]
    for i, image in enumerate(second):
        lanes = slice(i * leaf, (i + 1) * leaf)
        vec = vec_ref[:, lanes]
        first = first_ref[:, lanes]
        direction = grow * vec - step * first
        solution_ref[:, lanes] = step * vec + again * direction
        residual_ref[:, lanes] = (vec - step * first) - again * (grow * first - step * image)


def final_kernel(
    part_ref, group_ref, kgh_ref, kgl_ref, kah_ref, kal_ref, ubh_ref, ubl_ref, vec_ref,
    first_ref, solution_ref, residual_ref, rows_ref,
):
    second, share = second_image(
        part_ref, group_ref, kgh_ref, kgl_ref, ubh_ref, ubl_ref, rows_ref, (kah_ref, kal_ref)
    )
    update(group_ref, share, vec_ref, first_ref, second, solution_ref, residual_ref)


def last_kernel(
    part_ref, group_ref, kgh_ref, kgl_ref, ubh_ref, ubl_ref, second_ref, share_ref, rows_ref
):
    second, share = second_image(
        part_ref, group_ref, kgh_ref, kgl_ref, ubh_ref, ubl_ref, rows_ref, None
    )
    second_ref[...] = jnp.concatenate(second, axis=1)
    share_ref[...] = jnp.broadcast_to(share, share_ref.shape)


def update_kernel(
    group_ref, share_ref, vec_ref, first_ref, second_ref, solution_ref, residual_ref
):
    update(
        group_ref, share_ref[:, 0:1], vec_ref, first_ref, [second_ref[...]],
        solution_ref, residual_ref,
    )


def vmem(count):
    return [pl.BlockSpec(memory_space=pltpu.VMEM)] * count


def smem(count):
    return [pl.BlockSpec(memory_space=pltpu.SMEM)] * count


def shape(*dims, dtype=F32):
    return jax.ShapeDtypeStruct(dims, dtype)


def pair(*dims):
    return [shape(*dims, dtype=BF16)] * 2


def call(kernel, outs, args, scalars=0, scratch=(), flops=0):
    return pl.pallas_call(
        kernel,
        out_shape=tuple(outs),
        in_specs=smem(scalars) + vmem(len(args) - scalars),
        out_specs=tuple(vmem(len(outs))),
        scratch_shapes=[pltpu.VMEM(dims, F32) for dims in scratch],
        compiler_params=pltpu.CompilerParams(vmem_limit_bytes=GRANT),
        cost_estimate=pl.CostEstimate(
            flops=flops, transcendentals=0, bytes_accessed=1000000
        ),
    )(*args)


def swap(x, axis, m):
    return lax.ppermute(x, axis, [(i, i ^ m) for i in range(lax.axis_size(axis))])


def sides(m4):
    nodes = lax.axis_size("sub") * lax.axis_size("leaf")
    across = [(q, q + 1) for q in range(1, nodes - 1, 2)]
    across = across + [(target, source) for source, target in across]
    return lax.ppermute(m4, ("leaf", "sub"), across)


def spread_groups(held):
    held = held[None]
    for offsets in exchange_rounds(lax.axis_size("leaf")):
        held = jnp.concatenate([held] + [swap(held, "leaf", offset) for offset in offsets], axis=0)
    return held


def far_memory(*args):
    return [pltpu.with_memory_space_constraint(x, pltpu.HBM) for x in args]


def shards(
    probe_rhs,
    coords,
    near_list,
    far_leaf_list,
    far_group_list,
    leaf_basis,
    leaf_skeleton,
    leaf_transfer,
    device_transfer,
    group_skeleton,
):
    leaves, rank, leaf = leaf_basis.shape
    probes, count = probe_rhs.shape
    groups = lax.axis_size("leaf")
    subs = lax.axis_size("sub")
    half = REACH * leaf
    span = leaves * rank
    inside, across = window_tiles(leaves)
    transfer = leaf_transfer.reshape(span, rank)
    device = device_transfer[0]

    m1, own, m4, rhs, points, basis, transfer, device, near, far, group_rows = call(
        first_kernel,
        [
            shape(probes + 2 * EXTRA, span + half),
            shape(probes + 2 * EXTRA, span),
            shape(probes + EXTRA, half),
            shape(probes, count),
            shape(EXTRA, count),
            shape(leaves, rank, leaf),
            shape(span, rank),
            shape(rank, rank),
            shape(*near_list.shape, dtype=jnp.int32),
            shape(*far_leaf_list.shape, dtype=jnp.int32),
            shape(EXTRA, LANE),
        ],
        far_memory(
            far_group_list, probe_rhs, coords, leaf_skeleton, group_skeleton, leaf_basis,
            transfer, device, near_list, far_leaf_list,
        ),
        scalars=1,
    )
    r1, r2, r3 = swap(m1, "sub", 1), swap(own, "sub", 2), swap(own, "sub", 3)
    r4 = sides(m4)
    ubh, ubl = call(bases_kernel, pair(leaves, 2 * rank, leaf), (basis, transfer, device))
    th, tl = call(
        prepare_kernel, pair(len(inside) * leaf, leaf), (near, points), scratch=[(3, count, LANE)]
    )
    (term,) = call(term_kernel, [shape(probes // 2 + EXTRA, LANE)], (own, r1, r2, r3, group_rows))
    gathered = spread_groups(term)
    klh, kll = call(
        skeleton_kernel,
        pair(subs * span, span),
        (far, own, r1, r2, r3),
        scratch=[(subs, 3, span, LANE)],
    )
    hh, hl = call(
        border_kernel,
        pair(len(across) * leaf, leaf),
        (near, r1, r4, points),
        scratch=[(EXTRA, 2 * half), (3, 2 * half, LANE)],
    )
    (inner,) = call(inner_kernel, [shape(probes, count)], (rhs, th, tl))
    (part,) = call(
        outer_kernel,
        [shape(probes, count)],
        (inner, own, r1, r2, r3, r4, hh, hl, klh, kll, ubh, ubl),
    )
    image, kgh, kgl, m4 = call(
        middle_kernel,
        [shape(probes, count)] + pair(rank, groups * rank) + [shape(probes, half)],
        (part, gathered, ubh, ubl),
        scratch=[(EXTRA, groups * rank), (3, LANE, LANE)],
    )
    r4 = sides(m4)
    m1, own = call(
        second_kernel,
        [shape(probes + EXTRA, span + half), shape(probes + EXTRA, span)],
        (image, ubh, ubl),
    )
    r1, r2, r3 = swap(m1, "sub", 1), swap(own, "sub", 2), swap(own, "sub", 3)
    dense = groups * rank <= DENSE
    if dense:
        kah, kal = call(
            groups_kernel,
            pair(groups * rank, groups * rank),
            (gathered,),
            scratch=[(EXTRA, groups * rank), (3, groups * rank, LANE)],
        )
    inner, columns = call(
        again_kernel, [shape(probes, count), shape(probes, LANE)], (rhs, image, th, tl)
    )
    part, message = call(
        local_kernel,
        [
            shape(probes, count),
            shape(groups * subs, 1, probes // 2 // subs * LANE + SHARES * probes),
        ],
        (columns, image, inner, own, r1, r2, r3, r4, hh, hl, klh, kll, ubh, ubl),
    )
    gathered = lax.all_to_all(message, ("leaf", "sub"), 0, 0)
    outs = [shape(probes, count), shape(probes, count)]
    if dense:
        return call(
            final_kernel,
            outs,
            (part, gathered, kgh, kgl, kah, kal, ubh, ubl, rhs, image),
            scratch=[(groups, probes // 2, LANE)],
        )
    second, share = call(
        last_kernel,
        [shape(probes, count), shape(probes, LANE)],
        (part, gathered, kgh, kgl, ubh, ubl),
        scratch=[(groups, probes // 2, LANE)],
    )
    share = lax.psum(share, "leaf")
    return call(update_kernel, outs, (gathered, share, rhs, image, second))


def solution(mesh):
    return jax.shard_map(
        shards,
        mesh=mesh,
        in_specs=(
            P(None, ("leaf", "sub")),
            P(None, ("leaf", "sub")),
            P(("leaf", "sub"), None),
            P(("leaf", "sub"), None),
            P("leaf", None),
            P(("leaf", "sub"), None, None),
            P(None, ("leaf", "sub")),
            P(("leaf", "sub"), None, None),
            P(("leaf", "sub"), None, None),
            P(None, "leaf"),
        ),
        out_specs=(P(None, ("leaf", "sub")), P(None, ("leaf", "sub"))),
        check_vma=False,
    )
```
